128 devices in a mesh: group: 4 (over x), seq: 32 (over z, y, core).
Axes of the slice: x: 4, y: 4, z: 4, core: 2. Of those that a mesh axis runs over, the one named last changes fastest.
Arguments:
- tokens: bfloat16 [32, 2048, 2048], P('group', 'seq'), may hold values from -6 to 6
- image_keys: bfloat16 [32, 256, 2048], P('group', 'seq'), may hold values from -256 to 256
- image_values: bfloat16 [32, 256, 2048], P('group', 'seq'), may hold values from -18 to 18
- text_len: int32 [32], replicated, may hold values from 1 to 2048
- image_len: int32 [32], replicated, may hold values from 1 to 256
- counts: int32 [6], replicated, may hold values from 1 to 4, as said below
- old_group: int32 [6], replicated, may hold values from 0 to 3, as said below
- new_group: int32 [6], replicated, may hold values from 0 to 3, as said below
- w_query: bfloat16 [2048, 2048], replicated, may hold values from -0.125 to 0.125
- w_out: bfloat16 [2048, 2048], replicated, may hold values from -0.125 to 0.125
Outputs:
- layer_out: bfloat16 [32, 2048, 2048], P('group', 'seq')
The draws below stay inside these ranges and needn't reach their ends.
Inputs may be any that keep to these rules, and one draw needn't show every extreme that they name: `counts`: every task has at most 4 samples, and some task has exactly 4. `old_group`: each group is the old group of at most two tasks, and no two tasks share both their old group and their new group, so at most 4 samples go from one old group to one new group. `new_group`: each group is the new group of at most two tasks.
All inputs are finite; a program needn't handle non-finite values.
Results may differ from the reference program's by a relative error of at most 0.011.
Values may be sent and summed in bfloat16 or wider, within the bound.
No kernel may reach another device: no remote copies, remote signals or barrier semaphores. Data moves between devices by JAX's collectives and lax.ppermute only.
A program may use at most 128 MiB of HBM per device.

```python
import jax
import jax.numpy as jnp
from jax import lax

D = 2048
HEADS = 16
HEAD_DIM = 128
SAMPLE = 2048
IMG = 256
TASKS = 6
SLOTS = 8
HALF = 4
HH = 2048
TOTAL_SLOTS = 32
N_GROUP = 4


def draw_image_keys(key, part):
    drawn = jax.random.normal(jax.random.fold_in(key, 31), (N_GROUP * SLOTS, IMG, HEADS * HEAD_DIM), jnp.float32)
    drawn = jnp.clip(drawn, -6.0, 6.0)
    return drawn.astype(jnp.bfloat16)


def draw_counts(key, part):
    lowered = jax.random.randint(jax.random.fold_in(key, 5), (TASKS,), 0, 4, dtype=jnp.int32)
    smaller = jnp.maximum(HALF - 1, 1)
    drawn_counts = jnp.where(lowered == 0, smaller, HALF)
    chosen_task = jax.random.randint(jax.random.fold_in(key, 6), (), 0, TASKS, dtype=jnp.int32)
    task_ids = jnp.arange(TASKS, dtype=jnp.int32)
    return jnp.where(task_ids == chosen_task, HALF, drawn_counts).astype(jnp.int32)


def draw_old_group(key, part):
    shuffled = jax.random.permutation(jax.random.fold_in(key, 11), N_GROUP).astype(jnp.int32)
    task_ids = jnp.arange(TASKS, dtype=jnp.int32)
    return shuffled[task_ids % N_GROUP]


def draw_new_group(key, part):
    shuffled = jax.random.permutation(jax.random.fold_in(key, 23), N_GROUP).astype(jnp.int32)
    task_ids = jnp.arange(TASKS, dtype=jnp.int32)
    return shuffled[(task_ids + task_ids // N_GROUP) % N_GROUP]


def set_ends(values, stream_key, smallest, high):
    place = [jax.random.randint(jax.random.fold_in(stream_key, axis), (), 0, length) for axis, length in enumerate(values.shape)]
    widest = values.shape.index(max(values.shape))
    next_to = place[:widest] + [(place[widest] + 1) % values.shape[widest]] + place[widest + 1:]
    return values.at[tuple(place)].set(smallest).at[tuple(next_to)].set(high)


def level_of(rng, dims, split, smallest, high):
    def one(dim, blocks):
        heights = jax.random.uniform(jax.random.fold_in(jax.random.fold_in(rng, 6), dim), (blocks,), jnp.float32, smallest / len(split), high / len(split))
        return jnp.repeat(jnp.exp(heights), dims[dim] // blocks).reshape((-1,) + (1,) * (len(dims) - dim - 1))

    loudness = one(*split[0])
    for cut in split[1:]:
        loudness = loudness * one(*cut)
    return loudness


def bell_draw(own_key, shape, width, bound, cuts=(), kind=jnp.bfloat16):
    values = width * jax.random.normal(own_key, shape, jnp.float32)
    if cuts:
        values = values * level_of(own_key, shape, cuts, -0.22, 0.18)
    return jnp.clip(values, -bound, bound).astype(kind)


def setup_inputs(seed: int = 0) -> dict:
    seeds = jax.random.split(jax.random.key(seed), 11)
    tokens = bell_draw(seeds[0], (TOTAL_SLOTS, SAMPLE, D), 1.0, 6.0, ((0, 4), (1, 32)))
    image_keys = draw_image_keys(jax.random.fold_in(seeds[10], 71), 0)
    image_values = bell_draw(seeds[2], (TOTAL_SLOTS, IMG, HH), 3.0, 18.0, ((0, 4), (1, 32)))
    text_len = set_ends(jax.random.randint(seeds[3], (TOTAL_SLOTS,), 1, SAMPLE + 1), jax.random.fold_in(seeds[3], 1), 1, SAMPLE).astype(jnp.int32)
    image_len = set_ends(jax.random.randint(seeds[4], (TOTAL_SLOTS,), 1, IMG + 1), jax.random.fold_in(seeds[4], 1), 1, IMG).astype(jnp.int32)
    counts = draw_counts(jax.random.fold_in(seeds[10], 71), 0)
    old_group = draw_old_group(jax.random.fold_in(seeds[10], 71), 0)
    new_group = draw_new_group(jax.random.fold_in(seeds[10], 71), 0)
    w_query = bell_draw(seeds[8], (D, HH), D ** -0.5, 0.125)
    w_out = bell_draw(seeds[9], (HH, D), HH ** -0.5, 0.125)
    return dict(tokens=tokens, image_keys=image_keys, image_values=image_values, text_len=text_len, image_len=image_len, counts=counts, old_group=old_group, new_group=new_group, w_query=w_query, w_out=w_out)


masked_score = -1e+30
norm_eps = 1e-05

def layout(counts, old_group, new_group, group_count, slot_count):
    task_order = jnp.arange(counts.shape[0], dtype=jnp.int32)
    earlier = task_order[None, :] < task_order[:, None]
    same_old = old_group[None, :] == old_group[:, None]
    same_new = new_group[None, :] == new_group[:, None]
    old_start = lax.optimization_barrier(jnp.sum(jnp.where(earlier & same_old, counts[None, :], 0), axis=1)).astype(jnp.int32)
    new_start = lax.optimization_barrier(jnp.sum(jnp.where(earlier & same_new, counts[None, :], 0), axis=1)).astype(jnp.int32)
    target = jnp.arange(group_count * slot_count, dtype=jnp.int32)
    target_group = target // slot_count
    target_slot = target % slot_count
    matches = (new_group[None, :] == target_group[:, None]) & (target_slot[:, None] >= new_start[None, :]) & (target_slot[:, None] < (new_start + counts)[None, :])
    filled = jnp.any(matches, axis=1)
    offset = (target_slot - lax.optimization_barrier(jnp.sum(jnp.where(matches, new_start[None, :], 0), axis=1))).astype(jnp.int32)
    source_group = lax.optimization_barrier(jnp.sum(jnp.where(matches, old_group[None, :], 0), axis=1)).astype(jnp.int32)
    source_slot = (lax.optimization_barrier(jnp.sum(jnp.where(matches, old_start[None, :], 0), axis=1)) + offset).astype(jnp.int32)
    return (filled, source_group, source_slot, offset, old_start)

def normalize(samples_rows):
    values = samples_rows.astype(jnp.float32)
    average = lax.optimization_barrier(jnp.mean(values, axis=-1, keepdims=True))
    centred = values - average
    variance = lax.optimization_barrier(jnp.mean(centred * centred, axis=-1, keepdims=True))
    return (centred * lax.rsqrt(variance + norm_eps)).astype(jnp.bfloat16)

def reference(tokens, image_keys, image_values, text_len, image_len, counts, old_group, new_group, w_query, w_out):
    slot_count = tokens.shape[0] // N_GROUP
    score_scale = HEAD_DIM ** (-0.5)
    filled, source_group, source_slot, offset, old_start = layout(counts, old_group, new_group, N_GROUP, slot_count)

    def single_sample(inputs):
        sample_rows, key_rows, value_rows, limit_text, limit_key = inputs
        normal = normalize(sample_rows)
        queries = (jnp.dot(normal, w_query, preferred_element_type=jnp.float32) * score_scale).astype(jnp.bfloat16)
        head_queries = lax.optimization_barrier(queries).astype(jnp.float32).reshape(SAMPLE, HEADS, HEAD_DIM)
        head_keys = key_rows.astype(jnp.float32).reshape(IMG, HEADS, HEAD_DIM)
        head_values = value_rows.astype(jnp.float32).reshape(IMG, HEADS, HEAD_DIM)
        scores = jnp.einsum('qhd,khd->hqk', head_queries, head_keys)
        allowed = (jnp.arange(IMG, dtype=jnp.int32) < limit_key)[None, None, :]
        scores = jnp.where(allowed, scores, masked_score)
        row_max = lax.optimization_barrier(jnp.max(scores, axis=-1, keepdims=True))
        probs = jnp.where(allowed, jnp.exp(scores - row_max), 0.0)
        running_sum = lax.optimization_barrier(jnp.sum(probs, axis=-1))
        weights = lax.optimization_barrier(probs.astype(jnp.bfloat16)).astype(jnp.float32)
        context = jnp.einsum('hqk,khd->hqd', weights, head_values) / running_sum[..., None]
        context = context.transpose(1, 0, 2).reshape(SAMPLE, HEADS * HEAD_DIM).astype(jnp.bfloat16)
        projected = jnp.dot(context, w_out, preferred_element_type=jnp.float32)
        kept_rows = jnp.arange(SAMPLE, dtype=jnp.int32) < limit_text
        return jnp.where(kept_rows[:, None], projected, 0.0).astype(jnp.bfloat16)
    computed = lax.map(single_sample, (tokens, image_keys, image_values, text_len, image_len))
    source = jnp.where(filled, source_group * slot_count + source_slot, 0).astype(jnp.int32)
    picked = jnp.take(computed, source, axis=0)
    return jnp.where(filled[:, None, None], picked, jnp.zeros((), jnp.bfloat16))
```

```python
import functools

import jax
import jax.numpy as jnp
from jax import lax
from jax.experimental import pallas as pl
from jax.experimental.pallas import tpu as pltpu
from jax.sharding import PartitionSpec as P


HEADS = 16
HEAD_DIM = 128
WIDTH = 2048
GROUPS = 4
SLOTS = 8
HALF = 4
RING = 4
CORES = 2
ROWS = 64
KEYS = 8
IMG = 256

masked_score = -1e30
norm_eps = 1e-05


def seq_shift(axis, k):
    pairs = []
    for z in range(RING):
        for y in range(RING):
            for c in range(CORES):
                z2, y2, c2 = z, y, c
                if axis == "z":
                    z2 = (z + k) % RING
                elif axis == "y":
                    y2 = (y + k) % RING
                else:
                    c2 = 1 - c
                pairs.append(((z * RING + y) * CORES + c, (z2 * RING + y2) * CORES + c2))
    return pairs


def move_seq(a, axis, k=1):
    return lax.ppermute(a, "seq", seq_shift(axis, k))


def move_group(a, k):
    return lax.ppermute(a, "group", [(g, (g + k) % GROUPS) for g in range(GROUPS)])


def normalize(rows):
    values = rows.astype(jnp.float32)
    average = jnp.mean(values, axis=-1, keepdims=True)
    centred = values - average
    variance = jnp.mean(centred * centred, axis=-1, keepdims=True)
    return (centred * lax.rsqrt(variance + norm_eps)).astype(jnp.bfloat16)


def pick(pieces, which):
    out = pieces[0]
    for k in range(1, len(pieces)):
        out = jnp.where(which == k, pieces[k], out)
    return out


def attend_kernel(
    limit_ref, bias_ref, qm_ref, qt_ref, own_ref, prev_ref, next_ref, opa_ref, opb_ref, w_hbm,
    om_ref, ot_ref, ctx, w, sem,
):
    step = pl.program_id(0)
    copy = pltpu.make_async_copy(w_hbm, w, sem)

    @pl.when(step == 0)
    def _():
        copy.start()

    bias = bias_ref[0]
    row0 = pl.multiple_of(step * (2 * ROWS), 2 * ROWS)
    for h in range(HEADS):
        cols = slice(h * HEAD_DIM, (h + 1) * HEAD_DIM)

        def side(kv):
            return jnp.concatenate(
                [
                    ref[:, kv, :, cols].reshape(-1, HEAD_DIM)
                    for ref in (own_ref, prev_ref, next_ref, opa_ref, opb_ref)
                ],
                axis=0,
            )

        q = jnp.concatenate([qm_ref[0, :, cols], qt_ref[0, :, cols]], axis=0)
        scores = lax.dot_general(
            q, side(0), (((1,), (1,)), ((), ())), preferred_element_type=jnp.float32
        )
        scores = scores + bias
        top = jnp.max(scores, axis=-1, keepdims=True)
        probs = jnp.exp(scores - top)
        total = jnp.sum(probs, axis=-1, keepdims=True)
        mixed = jnp.dot(
            probs.astype(jnp.bfloat16), side(1), preferred_element_type=jnp.float32
        )
        ctx[pl.ds(row0, 2 * ROWS), cols] = (mixed / total).astype(jnp.bfloat16)

    @pl.when(step == 1)
    def _():
        copy.wait()
        row = lax.broadcasted_iota(jnp.int32, (ROWS, 1), 0)
        for n in range(4):
            cols = slice(n * 512, (n + 1) * 512)
            out = jnp.dot(ctx[...], w[:, cols], preferred_element_type=jnp.float32)
            for j in range(2):
                for side, ref in ((0, om_ref), (1, ot_ref)):
                    at = (2 * j + side) * ROWS
                    kept = row < limit_ref[j, side]
                    ref[j, :, cols] = jnp.where(kept, out[at : at + ROWS], 0.0).astype(
                        jnp.bfloat16
                    )


def attend(limit, bias, q_mine, q_theirs, pieces, w_out):
    own, prev, after, opa, opb = pieces

    def kv_spec(n):
        return pl.BlockSpec((n, 2, None, 16, WIDTH), lambda j: (0, 0, j, 0, 0))

    q_spec = pl.BlockSpec((1, ROWS, WIDTH), lambda j: (j, 0, 0))
    o_spec = pl.BlockSpec((2, ROWS, WIDTH), lambda j: (0, 0, 0))
    out = jax.ShapeDtypeStruct((2, ROWS, WIDTH), jnp.bfloat16)
    return pl.pallas_call(
        attend_kernel,
        out_shape=(out, out),
        grid=(2,),
        in_specs=[
            pl.BlockSpec(memory_space=pltpu.SMEM),
            pl.BlockSpec((1, 1, IMG), lambda j: (j, 0, 0)),
            q_spec,
            q_spec,
            kv_spec(4),
            kv_spec(4),
            kv_spec(4),
            kv_spec(2),
            kv_spec(2),
            pl.BlockSpec(memory_space=pl.ANY),
        ],
        out_specs=(o_spec, o_spec),
        scratch_shapes=[
            pltpu.VMEM((4 * ROWS, WIDTH), jnp.bfloat16),
            pltpu.VMEM((WIDTH, WIDTH), jnp.bfloat16),
            pltpu.SemaphoreType.DMA,
        ],
        compiler_params=pltpu.CompilerParams(
            dimension_semantics=("arbitrary",), vmem_limit_bytes=32 * 2**20
        ),
        cost_estimate=pl.CostEstimate(
            flops=3_500_000_000, bytes_accessed=14_000_000, transcendentals=1_000_000
        ),
    )(limit, bias, q_mine, q_theirs, own, prev, after, opa, opb, w_out)


def place_kernel(index_ref, m0_ref, m1_ref, t0_ref, t1_ref, out_ref):
    slot = pl.program_id(0)
    source = index_ref[slot]
    for n, ref in enumerate((m0_ref, m1_ref, t0_ref, t1_ref)):
        for j in range(2):

            @pl.when(source == 2 * n + j)
            def _():
                out_ref[0] = ref[j]

    @pl.when(source < 0)
    def _():
        out_ref[0] = jnp.zeros((ROWS, WIDTH), jnp.bfloat16)


def place(index, m0, m1, t0, t1):
    whole = pl.BlockSpec((2, ROWS, WIDTH), lambda s, i: (0, 0, 0))
    return pl.pallas_call(
        place_kernel,
        out_shape=jax.ShapeDtypeStruct((SLOTS, ROWS, WIDTH), jnp.bfloat16),
        grid_spec=pltpu.PrefetchScalarGridSpec(
            num_scalar_prefetch=1,
            grid=(SLOTS,),
            in_specs=[whole] * 4,
            out_specs=pl.BlockSpec((1, ROWS, WIDTH), lambda s, i: (s, 0, 0)),
        ),
        cost_estimate=pl.CostEstimate(
            flops=1_000_000, bytes_accessed=4_000_000, transcendentals=0
        ),
    )(index, m0, m1, t0, t1)


def on_device(
    tokens, image_keys, image_values, text_len, image_len, counts, old_group, new_group, w_query, w_out
):
    group = lax.axis_index("group")
    d = lax.axis_index("seq")
    core = d % CORES
    y = (d // CORES) % RING
    z = d // (CORES * RING)

    order = jnp.arange(counts.shape[0], dtype=jnp.int32)
    earlier = order[None, :] < order[:, None]
    same_old = old_group[None, :] == old_group[:, None]
    same_new = new_group[None, :] == new_group[:, None]
    old_start = jnp.sum(jnp.where(earlier & same_old, counts[None, :], 0), axis=1)
    rank = jnp.sum(jnp.where(earlier & same_new, 1, 0), axis=1)
    steps = jnp.arange(GROUPS, dtype=jnp.int32)
    outgoing = (old_group[None, :] == group) & (
        new_group[None, :] == ((group + steps) % GROUPS)[:, None]
    )
    first = jnp.sum(jnp.where(outgoing, old_start[None, :], 0), axis=1)
    ranks = jnp.arange(2, dtype=jnp.int32)
    mine = (new_group[None, :] == group) & (rank[None, :] == ranks[:, None])
    came = jnp.sum(jnp.where(mine, ((group - old_group) % GROUPS)[None, :], 0), axis=1)
    amount = jnp.sum(jnp.where(mine, counts[None, :], 0), axis=1)
    base = jnp.sum(jnp.where(mine, (old_group * SLOTS + old_start)[None, :], 0), axis=1)

    sample = 2 * core + jnp.arange(2, dtype=jnp.int32)
    there = sample[None, :] < amount[:, None]
    old_slot = jnp.where(there, base[:, None] + sample[None, :], 0)
    hot = old_slot[:, :, None] == jnp.arange(text_len.shape[0], dtype=jnp.int32)
    text_limit = jnp.where(there, jnp.sum(jnp.where(hot, text_len, 0), axis=-1), 0)
    key_limit = jnp.where(there, jnp.sum(jnp.where(hot, image_len, 0), axis=-1), IMG)
    row_first = jnp.stack([d, d + 1 - 2 * core]) * ROWS
    limit = text_limit[:, :, None] - row_first[None, None, :]

    def kv_of(k):
        return jnp.stack(
            [
                lax.dynamic_slice_in_dim(image_keys, first[k], HALF),
                lax.dynamic_slice_in_dim(image_values, first[k], HALF),
            ]
        )

    kv = [kv_of(0)] + [move_group(kv_of(k), k) for k in (1, 2, 3)]
    kv = [pick(kv, came[r]) for r in range(2)]

    normal = normalize(tokens).reshape(SLOTS * ROWS, WIDTH)
    queries = (
        jnp.dot(normal, w_query, preferred_element_type=jnp.float32) * HEAD_DIM ** (-0.5)
    ).astype(jnp.bfloat16)
    queries = queries.reshape(SLOTS, ROWS, WIDTH)

    kv_mine = [lax.dynamic_slice_in_dim(a, 2 * core, 2, axis=1) for a in kv]
    kv_send = jnp.stack([lax.dynamic_slice_in_dim(a, 2 - 2 * core, 2, axis=1) for a in kv])
    kv_theirs = move_seq(kv_send, "c")
    block = [jnp.concatenate([kv_mine[r], kv_theirs[r]], axis=2) for r in range(2)]

    quarter = []
    for r, axis in ((0, "z"), (1, "y")):
        quarter.append(
            jnp.stack([block[r]] + [move_seq(block[r], axis, k) for k in (1, 2, 3)])
        )

    def q_of(k):
        return lax.dynamic_slice_in_dim(queries, first[k], HALF)

    q = [q_of(0)] + [move_group(q_of(k), k) for k in (1, 2, 3)]
    q_mine, q_send = [], []
    for r in range(2):
        q_mine.append(
            pick([lax.dynamic_slice_in_dim(a, 2 * core, 2) for a in q], came[r])
        )
        q_send.append(
            pick([lax.dynamic_slice_in_dim(a, 2 - 2 * core, 2) for a in q], came[r])
        )
    q_theirs = [move_seq(a, "c") for a in q_send]

    pieces = []
    for r, axis in ((0, "y"), (1, "z")):
        own = quarter[r]
        prev = move_seq(own, axis, 1)
        after = move_seq(own, axis, 3)
        opa = move_seq(prev[:2], axis, 1)
        opb = move_seq(after[2:], axis, 3)
        pieces.append((own, prev, after, opa, opb))

    i = jnp.arange(IMG, dtype=jnp.int32)
    run = i // 64
    which = (i // 16) % 4
    within = i % 16
    within = within % 8 + 8 * jnp.where(within < 8, core, 1 - core)
    hop = jnp.array([0, -1, 1, 2], jnp.int32)[run]
    key_at = [
        64 * ((z - which) % RING) + 16 * ((y + hop) % RING) + within,
        64 * ((z + hop) % RING) + 16 * ((y - which) % RING) + within,
    ]

    done = []
    for r in range(2):
        allowed = key_at[r][None, :] < key_limit[r][:, None]
        bias = jnp.where(allowed, 0.0, masked_score).astype(jnp.float32)[:, None, :]
        out_mine, out_send = attend(limit[r], bias, q_mine[r], q_theirs[r], pieces[r], w_out)
        done.append((out_mine, move_seq(out_send, "c")))

    slot = jnp.arange(SLOTS, dtype=jnp.int32)
    second = (slot >= amount[0]).astype(jnp.int32)
    j = slot - second * amount[0]
    filled = slot < amount[0] + amount[1]
    index = jnp.where(j // 2 == core, 0, 4) + 2 * second + j % 2
    index = jnp.where(filled, index, -1)
    return place(index, done[0][0], done[1][0], done[0][1], done[1][1])


def solution(mesh):
    split = P("group", "seq", None)
    return jax.shard_map(
        on_device,
        mesh=mesh,
        in_specs=(split,) * 3 + (P(),) * 7,
        out_specs=split,
        check_vma=False,
    )
```

```python
import functools

import jax
import jax.numpy as jnp
from jax import lax
from jax.experimental import pallas as pl
from jax.experimental.pallas import tpu as pltpu
from jax.sharding import PartitionSpec as P


HEADS = 16
HEAD_DIM = 128
WIDTH = 2048
GROUPS = 4
SLOTS = 8
TASKS = 6
HALF = 4
RING = 4
CORES = 2
ROWS = 64
KEYS = 8
IMG = 256

masked_score = -1e30
norm_eps = 1e-05


def seq_shift(axis, k):
    pairs = []
    for z in range(RING):
        for y in range(RING):
            for c in range(CORES):
                z2, y2, c2 = z, y, c
                if axis == "z":
                    z2 = (z + k) % RING
                elif axis == "y":
                    y2 = (y + k) % RING
                else:
                    c2 = 1 - c
                pairs.append(((z * RING + y) * CORES + c, (z2 * RING + y2) * CORES + c2))
    return pairs


def move_seq(a, axis, k=1):
    return lax.ppermute(a, "seq", seq_shift(axis, k))


def move_group(a, k):
    return lax.ppermute(a, "group", [(g, (g + k) % GROUPS) for g in range(GROUPS)])


def pack_kernel(
    counts_ref, old_ref, new_ref, text_ref, image_ref, k_ref, v_ref,
    kv0_ref, kv1_ref, kv2_ref, kv3_ref, first_ref, came_ref, head0_ref, head1_ref, index_ref, sem,
):
    group, d = lax.axis_index("group"), lax.axis_index("seq")
    core = d % CORES
    y = (d // CORES) % RING
    z = d // (CORES * RING)
    tasks = range(TASKS)
    count = [counts_ref[t] for t in tasks]
    old = [old_ref[t] for t in tasks]
    new = [new_ref[t] for t in tasks]
    zero = jnp.int32(0)
    start, rank = [], []
    for t in tasks:
        at, before = zero, zero
        for u in range(t):
            at = at + jnp.where(old[u] == old[t], count[u], 0)
            before = before + jnp.where(new[u] == new[t], 1, 0)
        start.append(at)
        rank.append(before)
    copies = []
    for k, out in enumerate((kv0_ref, kv1_ref, kv2_ref, kv3_ref)):
        first = zero
        for t in tasks:
            goes = (old[t] == group) & (new[t] == (group + k) % GROUPS)
            first = jnp.where(goes, start[t], first)
        first_ref[k] = first
        for i, ref in enumerate((k_ref, v_ref)):
            copies.append(
                pltpu.make_async_copy(ref.at[pl.ds(first, HALF)], out.at[i], sem.at[2 * k + i])
            )
            copies[-1].start()
    amounts = []
    for r, head in enumerate((head0_ref, head1_ref)):
        came, amount, base = zero, zero, zero
        for t in tasks:
            mine = (new[t] == group) & (rank[t] == r)
            came = jnp.where(mine, (group - old[t] + GROUPS) % GROUPS, came)
            amount = jnp.where(mine, count[t], amount)
            base = jnp.where(mine, old[t] * SLOTS + start[t], base)
        came_ref[r] = came
        amounts.append(amount)
        head[0], head[1], head[2] = z, y, core
        for j in range(2):
            sample = 2 * core + j
            there = sample < amount
            slot = jnp.where(there, base + sample, 0)
            head[3 + j] = jnp.where(there, image_ref[slot], IMG)
            text = jnp.where(there, text_ref[slot], 0)
            head[5 + 2 * j] = text - d * ROWS
            head[6 + 2 * j] = text - (d + 1 - 2 * core) * ROWS
    for slot in range(SLOTS):
        second = jnp.where(slot >= amounts[0], 1, 0)
        j = slot - second * amounts[0]
        at = jnp.where(j // 2 == core, 0, 4) + 2 * second + j % 2
        index_ref[slot] = jnp.where(slot < amounts[0] + amounts[1], at, -1)
    for copy in copies:
        copy.wait()


def pack(counts, old_group, new_group, text_len, image_len, keys, values):
    smem = pl.BlockSpec(memory_space=pltpu.SMEM)
    vmem = pl.BlockSpec(memory_space=pltpu.VMEM)
    kv = jax.ShapeDtypeStruct((2, HALF, KEYS, WIDTH), jnp.bfloat16)
    ints = [jax.ShapeDtypeStruct((n,), jnp.int32) for n in (4, 2, 9, 9, 8)]
    return pl.pallas_call(
        pack_kernel,
        out_shape=(kv,) * 4 + tuple(ints),
        in_specs=[smem] * 5 + [pl.BlockSpec(memory_space=pltpu.HBM)] * 2,
        out_specs=(vmem,) * 4 + (smem,) * 5,
        scratch_shapes=[pltpu.SemaphoreType.DMA((8,))],
        cost_estimate=pl.CostEstimate(flops=1_000_000, bytes_accessed=2_000_000, transcendentals=0),
    )(counts, old_group, new_group, text_len, image_len, keys, values)


def choose_kernel(came_ref, kv0_ref, kv1_ref, kv2_ref, kv3_ref, mine_ref, send_ref, sem):
    core = lax.axis_index("seq") % CORES
    for r in range(2):
        for k, ref in enumerate((kv0_ref, kv1_ref, kv2_ref, kv3_ref)):

            @pl.when(came_ref[r] == k)
            def _():
                for side, (at, out) in enumerate(((2 * core, mine_ref), (2 - 2 * core, send_ref))):
                    pltpu.make_async_copy(
                        ref.at[:, pl.ds(at, 2)], out.at[r], sem.at[r, side]
                    ).start()

    for r in range(2):
        for side, out in enumerate((mine_ref, send_ref)):
            pltpu.make_async_copy(kv0_ref.at[:, pl.ds(0, 2)], out.at[r], sem.at[r, side]).wait()


def choose(came, parts):
    out = jax.ShapeDtypeStruct((2, 2, 2, KEYS, WIDTH), jnp.bfloat16)
    return pl.pallas_call(
        choose_kernel,
        out_shape=(out, out),
        in_specs=[pl.BlockSpec(memory_space=pltpu.SMEM)] + [pl.BlockSpec(memory_space=pl.ANY)] * 4,
        out_specs=(pl.BlockSpec(memory_space=pltpu.VMEM),) * 2,
        scratch_shapes=[pltpu.SemaphoreType.DMA((2, 2))],
        cost_estimate=pl.CostEstimate(flops=1_000_000, bytes_accessed=1_000_000, transcendentals=0),
    )(came, *parts)


def spread_kernel(first_ref, x_ref, o0_ref, o1_ref, o2_ref, o3_ref, sem):
    copies = [
        pltpu.make_async_copy(x_ref.at[pl.ds(first_ref[k], HALF)], out, sem.at[k])
        for k, out in enumerate((o0_ref, o1_ref, o2_ref, o3_ref))
    ]
    for copy in copies:
        copy.start()
    for copy in copies:
        copy.wait()


def spread(first, tokens):
    out = jax.ShapeDtypeStruct((HALF, ROWS, WIDTH), jnp.bfloat16)
    return pl.pallas_call(
        spread_kernel,
        out_shape=(out,) * 4,
        in_specs=[pl.BlockSpec(memory_space=pltpu.SMEM), pl.BlockSpec(memory_space=pltpu.HBM)],
        out_specs=(pl.BlockSpec(memory_space=pltpu.VMEM),) * 4,
        scratch_shapes=[pltpu.SemaphoreType.DMA((4,))],
        cost_estimate=pl.CostEstimate(flops=1_000_000, bytes_accessed=8_000_000, transcendentals=0),
    )(first, tokens)


def project_kernel(
    came_ref, head_ref, x0_ref, x1_ref, x2_ref, x3_ref, w_ref, mine_ref, send_ref, x, normal, sem,
):
    step = pl.program_id(0)
    core = head_ref[2]

    @pl.when(step == 0)
    def _():
        for r in range(2):
            for k, ref in enumerate((x0_ref, x1_ref, x2_ref, x3_ref)):

                @pl.when(came_ref[r] == k)
                def _():
                    for side, at in ((0, 2 * core), (1, 2 - 2 * core)):
                        pltpu.make_async_copy(
                            ref.at[pl.ds(at, 2)], x.at[pl.ds(4 * side + 2 * r, 2)], sem.at[r, side]
                        ).start()

        for r in range(2):
            for side in range(2):
                pltpu.make_async_copy(
                    x0_ref.at[pl.ds(0, 2)], x.at[pl.ds(4 * side + 2 * r, 2)], sem.at[r, side]
                ).wait()

        def one(i, carry):
            values = x[i].astype(jnp.float32)
            centred = values - jnp.mean(values, axis=-1, keepdims=True)
            variance = jnp.mean(centred * centred, axis=-1, keepdims=True)
            at = pl.multiple_of(i * ROWS, ROWS)
            normal[pl.ds(at, ROWS), :] = (centred * lax.rsqrt(variance + norm_eps)).astype(
                jnp.bfloat16
            )
            return carry

        lax.fori_loop(0, SLOTS, one, 0)

    out = jnp.dot(normal[...], w_ref[...], preferred_element_type=jnp.float32)
    out = (out * HEAD_DIM ** (-0.5)).astype(jnp.bfloat16)
    out = out.reshape(2, 4, ROWS, out.shape[-1])
    mine_ref[...] = out[0]
    send_ref[...] = out[1]


def project(came, head, parts, w_query):
    cols = 512
    smem = pl.BlockSpec(memory_space=pltpu.SMEM)
    out = jax.ShapeDtypeStruct((4, ROWS, WIDTH), jnp.bfloat16)
    o_spec = pl.BlockSpec((4, ROWS, cols), lambda n: (0, 0, n))
    return pl.pallas_call(
        project_kernel,
        out_shape=(out, out),
        grid=(WIDTH // cols,),
        in_specs=[smem, smem]
        + [pl.BlockSpec(memory_space=pl.ANY)] * 4
        + [pl.BlockSpec((WIDTH, cols), lambda n: (0, n))],
        out_specs=(o_spec, o_spec),
        scratch_shapes=[
            pltpu.VMEM((SLOTS, ROWS, WIDTH), jnp.bfloat16),
            pltpu.VMEM((SLOTS * ROWS, WIDTH), jnp.bfloat16),
            pltpu.SemaphoreType.DMA((2, 2)),
        ],
        compiler_params=pltpu.CompilerParams(
            dimension_semantics=("arbitrary",), vmem_limit_bytes=24 * 2**20
        ),
        cost_estimate=pl.CostEstimate(
            flops=4_300_000_000, bytes_accessed=14_000_000, transcendentals=0
        ),
    )(came, head, *parts, w_query)


def attend_kernel(
    rank, head_ref, qm_ref, qt_ref, own_ref, prev_ref, next_ref, opa_ref, opb_ref, w_hbm,
    om_ref, ot_ref, ctx, w, sem,
):
    step = pl.program_id(0)
    copy = pltpu.make_async_copy(w_hbm, w, sem)

    @pl.when(step == 0)
    def _():
        copy.start()

    z, y, core = head_ref[0], head_ref[1], head_ref[2]
    key_limit = jnp.where(step == 0, head_ref[3], head_ref[4])
    i = lax.broadcasted_iota(jnp.int32, (1, IMG), 1)
    run, which, within = i // 64, (i // 16) & 3, i & 15
    hop = jnp.where(run == 1, 3, jnp.where(run == 2, 1, jnp.where(run == 3, 2, 0)))
    back = 4 - which
    at_z = (z + (back if rank == 0 else hop)) & 3
    at_y = (y + (hop if rank == 0 else back)) & 3
    within = (within & 7) + 8 * jnp.where(within < 8, core, 1 - core)
    bias = jnp.where(64 * at_z + 16 * at_y + within < key_limit, 0.0, masked_score)
    row0 = pl.multiple_of(step * (2 * ROWS), 2 * ROWS)
    for h in range(HEADS):
        cols = slice(h * HEAD_DIM, (h + 1) * HEAD_DIM)

        def side(kv):
            return jnp.concatenate(
                [
                    ref[:, kv, :, cols].reshape(-1, HEAD_DIM)
                    for ref in (own_ref, prev_ref, next_ref, opa_ref, opb_ref)
                ],
                axis=0,
            )

        q = jnp.concatenate([qm_ref[0, :, cols], qt_ref[0, :, cols]], axis=0)
        scores = lax.dot_general(
            q, side(0), (((1,), (1,)), ((), ())), preferred_element_type=jnp.float32
        )
        scores = scores + bias
        top = jnp.max(scores, axis=-1, keepdims=True)
        probs = jnp.exp(scores - top)
        total = jnp.sum(probs, axis=-1, keepdims=True)
        mixed = jnp.dot(
            probs.astype(jnp.bfloat16), side(1), preferred_element_type=jnp.float32
        )
        ctx[pl.ds(row0, 2 * ROWS), cols] = (mixed / total).astype(jnp.bfloat16)

    @pl.when(step == 1)
    def _():
        copy.wait()
        row = lax.broadcasted_iota(jnp.int32, (ROWS, 1), 0)
        for n in range(4):
            cols = slice(n * 512, (n + 1) * 512)
            out = jnp.dot(ctx[...], w[:, cols], preferred_element_type=jnp.float32)
            for j in range(2):
                for side, ref in ((0, om_ref), (1, ot_ref)):
                    at = (2 * j + side) * ROWS
                    kept = row < head_ref[5 + 2 * j + side]
                    ref[j, :, cols] = jnp.where(kept, out[at : at + ROWS], 0.0).astype(
                        jnp.bfloat16
                    )


def attend(rank, head, q_mine, q_theirs, pieces, w_out):
    own, prev, after, opa, opb = pieces

    def kv_spec(n):
        return pl.BlockSpec((n, 2, None, 16, WIDTH), lambda j: (0, 0, j, 0, 0))

    q_spec = pl.BlockSpec((1, ROWS, WIDTH), lambda j: (2 * rank + j, 0, 0))
    o_spec = pl.BlockSpec((2, ROWS, WIDTH), lambda j: (0, 0, 0))
    out = jax.ShapeDtypeStruct((2, ROWS, WIDTH), jnp.bfloat16)
    return pl.pallas_call(
        functools.partial(attend_kernel, rank),
        out_shape=(out, out),
        grid=(2,),
        in_specs=[
            pl.BlockSpec(memory_space=pltpu.SMEM),
            q_spec,
            q_spec,
            kv_spec(4),
            kv_spec(4),
            kv_spec(4),
            kv_spec(2),
            kv_spec(2),
            pl.BlockSpec(memory_space=pltpu.HBM),
        ],
        out_specs=(o_spec, o_spec),
        scratch_shapes=[
            pltpu.VMEM((4 * ROWS, WIDTH), jnp.bfloat16),
            pltpu.VMEM((WIDTH, WIDTH), jnp.bfloat16),
            pltpu.SemaphoreType.DMA,
        ],
        compiler_params=pltpu.CompilerParams(
            dimension_semantics=("arbitrary",), vmem_limit_bytes=32 * 2**20
        ),
        cost_estimate=pl.CostEstimate(
            flops=3_500_000_000, bytes_accessed=14_000_000, transcendentals=1_000_000
        ),
    )(head, q_mine, q_theirs, own, prev, after, opa, opb, w_out)


def place_kernel(index_ref, m0_ref, m1_ref, t0_ref, t1_ref, out_ref, zeros, sem):
    zeros[...] = jnp.zeros_like(zeros)
    for slot in range(SLOTS):
        source = index_ref[slot]
        for n, ref in enumerate((m0_ref, m1_ref, t0_ref, t1_ref)):
            for j in range(2):

                @pl.when(source == 2 * n + j)
                def _():
                    pltpu.make_async_copy(ref.at[j], out_ref.at[slot], sem.at[slot]).start()

        @pl.when(source < 0)
        def _():
            pltpu.make_async_copy(zeros, out_ref.at[slot], sem.at[slot]).start()

    for slot in range(SLOTS):
        pltpu.make_async_copy(zeros, out_ref.at[slot], sem.at[slot]).wait()


def place(index, m0, m1, t0, t1):
    return pl.pallas_call(
        place_kernel,
        out_shape=jax.ShapeDtypeStruct((SLOTS, ROWS, WIDTH), jnp.bfloat16),
        in_specs=[pl.BlockSpec(memory_space=pltpu.SMEM)]
        + [pl.BlockSpec(memory_space=pltpu.VMEM)] * 4,
        out_specs=pl.BlockSpec(memory_space=pl.ANY),
        scratch_shapes=[
            pltpu.VMEM((ROWS, WIDTH), jnp.bfloat16),
            pltpu.SemaphoreType.DMA((SLOTS,)),
        ],
        compiler_params=pltpu.CompilerParams(vmem_limit_bytes=8 * 2**20),
        cost_estimate=pl.CostEstimate(
            flops=1_000_000, bytes_accessed=4_000_000, transcendentals=0
        ),
    )(index, m0, m1, t0, t1)


def compute(
    tokens, image_keys, image_values, text_len, image_len, counts, old_group, new_group, w_query, w_out
):
    *kv, first, came, head0, head1, index = pack(
        counts, old_group, new_group, text_len, image_len, image_keys, image_values
    )

    for k in (2, 1, 3):
        kv[k] = move_group(kv[k], k)
    x = list(spread(first, tokens))
    for k in (2, 1, 3):
        x[k] = move_group(x[k], k)

    kv_mine, kv_send = choose(came, kv)
    kv_theirs = move_seq(kv_send, "c")
    block = [jnp.concatenate([kv_mine[r], kv_theirs[r]], axis=2) for r in range(2)]

    quarter = []
    for r, axis in ((0, "z"), (1, "y")):
        parts = [block[r]]
        for k in (1, 2, 3):
            parts.append(move_seq(block[r], axis, k))
        quarter.append(jnp.stack(parts))

    pieces = []
    for r, axis in ((0, "y"), (1, "z")):
        own = quarter[r]
        prev = move_seq(own, axis, 1)
        after = move_seq(own, axis, 3)
        opa = move_seq(prev[:2], axis, 1)
        opb = move_seq(after[2:], axis, 3)
        pieces.append((own, prev, after, opa, opb))

    q_mine, q_send = project(came, head0, x, w_query)
    q_theirs = move_seq(q_send, "c")

    done = []
    for r, head in enumerate((head0, head1)):
        out_mine, out_send = attend(r, head, q_mine, q_theirs, pieces[r], w_out)
        done.append((out_mine, move_seq(out_send, "c")))
    return place(index, done[0][0], done[1][0], done[0][1], done[1][1])


def solution(mesh):
    split = P("group", "seq", None)
    return jax.shard_map(
        compute,
        mesh=mesh,
        in_specs=(split,) * 3 + (P(),) * 7,
        out_specs=split,
        check_vma=False,
    )
```

```python
import functools

import jax
import jax.numpy as jnp
from jax import lax
from jax.experimental import pallas as pl
from jax.experimental.pallas import tpu as pltpu
from jax.sharding import PartitionSpec as P


HEADS = 16
HEAD_DIM = 128
WIDTH = 2048
GROUPS = 4
SLOTS = 8
TASKS = 6
HALF = 4
RING = 4
CORES = 2
ROWS = 64
PART = 32
KEYS = 8
IMG = 256

masked_score = -1e30
norm_eps = 1e-05


def seq_moves(phase, k):
    pairs = []
    for z in range(RING):
        for y in range(RING):
            for c in range(CORES):
                z2, y2, c2 = z, y, c
                if phase == "swap":
                    c2 = 1 - c
                elif (phase == "near") == (c == 0):
                    z2 = (z + k) % RING
                else:
                    y2 = (y + k) % RING
                pairs.append(((z * RING + y) * CORES + c, (z2 * RING + y2) * CORES + c2))
    return pairs


def move_seq(a, phase, k=1):
    return lax.ppermute(a, "seq", seq_moves(phase, k))


def move_group(a, k):
    return lax.ppermute(a, "group", [(g, (g + k) % GROUPS) for g in range(GROUPS)])


def pack_kernel(
    counts_ref, old_ref, new_ref, text_ref, image_ref, k_ref, v_ref,
    kv0_ref, kv1_ref, kv2_ref, kv3_ref, first_ref, came_ref, head0_ref, head1_ref, index_ref, sem,
):
    group, d = lax.axis_index("group"), lax.axis_index("seq")
    core = d % CORES
    y = (d // CORES) % RING
    z = d // (CORES * RING)
    tasks = range(TASKS)
    count = [counts_ref[t] for t in tasks]
    old = [old_ref[t] for t in tasks]
    new = [new_ref[t] for t in tasks]
    zero = jnp.int32(0)
    start, rank = [], []
    for t in tasks:
        at, before = zero, zero
        for u in range(t):
            at = at + jnp.where(old[u] == old[t], count[u], 0)
            before = before + jnp.where(new[u] == new[t], 1, 0)
        start.append(at)
        rank.append(before)
    copies = []
    for k, out in enumerate((kv0_ref, kv1_ref, kv2_ref, kv3_ref)):
        first = zero
        for t in tasks:
            goes = (old[t] == group) & (new[t] == (group + k) % GROUPS)
            first = jnp.where(goes, start[t], first)
        first_ref[k] = first
        for i, ref in enumerate((k_ref, v_ref)):
            copies.append(
                pltpu.make_async_copy(ref.at[pl.ds(first, HALF)], out.at[i], sem.at[2 * k + i])
            )
            copies[-1].start()
    amounts = []
    for r, head in enumerate((head0_ref, head1_ref)):
        came, amount, base = zero, zero, zero
        for t in tasks:
            mine = (new[t] == group) & (rank[t] == r)
            came = jnp.where(mine, (group - old[t] + GROUPS) % GROUPS, came)
            amount = jnp.where(mine, count[t], amount)
            base = jnp.where(mine, old[t] * SLOTS + start[t], base)
        came_ref[r] = came
        amounts.append(amount)
        head[0], head[1], head[2] = z, y, core
        for j in range(2):
            sample = 2 * core + j
            there = sample < amount
            slot = jnp.where(there, base + sample, 0)
            head[3 + j] = jnp.where(there, image_ref[slot], IMG)
            text = jnp.where(there, text_ref[slot], 0)
            head[5 + 2 * j] = text - d * ROWS
            head[6 + 2 * j] = text - (d + 1 - 2 * core) * ROWS
    for slot in range(SLOTS):
        second = jnp.where(slot >= amounts[0], 1, 0)
        j = slot - second * amounts[0]
        at = jnp.where(j // 2 == core, 0, 4) + 2 * second + j % 2
        index_ref[slot] = jnp.where(slot < amounts[0] + amounts[1], at, -1)
    for copy in copies:
        copy.wait()


def pack(counts, old_group, new_group, text_len, image_len, keys, values):
    smem = pl.BlockSpec(memory_space=pltpu.SMEM)
    vmem = pl.BlockSpec(memory_space=pltpu.VMEM)
    kv = jax.ShapeDtypeStruct((2, HALF, KEYS, WIDTH), jnp.bfloat16)
    ints = [jax.ShapeDtypeStruct((n,), jnp.int32) for n in (4, 2, 9, 9, 8)]
    return pl.pallas_call(
        pack_kernel,
        out_shape=(kv,) * 4 + tuple(ints),
        in_specs=[smem] * 5 + [pl.BlockSpec(memory_space=pltpu.HBM)] * 2,
        out_specs=(vmem,) * 4 + (smem,) * 5,
        scratch_shapes=[pltpu.SemaphoreType.DMA((8,))],
        cost_estimate=pl.CostEstimate(flops=1_000_000, bytes_accessed=2_000_000, transcendentals=0),
    )(counts, old_group, new_group, text_len, image_len, keys, values)


def choose_kernel(came_ref, kv0_ref, kv1_ref, kv2_ref, kv3_ref, mine_ref, send_ref, sem):
    core = lax.axis_index("seq") % CORES
    for r in range(2):
        for k, ref in enumerate((kv0_ref, kv1_ref, kv2_ref, kv3_ref)):

            @pl.when(came_ref[r] == k)
            def _():
                for side, (at, out) in enumerate(((2 * core, mine_ref), (2 - 2 * core, send_ref))):
                    pltpu.make_async_copy(
                        ref.at[:, pl.ds(at, 2)], out.at[r], sem.at[r, side]
                    ).start()

    for r in range(2):
        for side, out in enumerate((mine_ref, send_ref)):
            pltpu.make_async_copy(kv0_ref.at[:, pl.ds(0, 2)], out.at[r], sem.at[r, side]).wait()


def choose(came, parts):
    out = jax.ShapeDtypeStruct((2, 2, 2, KEYS, WIDTH), jnp.bfloat16)
    return pl.pallas_call(
        choose_kernel,
        out_shape=(out, out),
        in_specs=[pl.BlockSpec(memory_space=pltpu.SMEM)] + [pl.BlockSpec(memory_space=pl.ANY)] * 4,
        out_specs=(pl.BlockSpec(memory_space=pltpu.VMEM),) * 2,
        scratch_shapes=[pltpu.SemaphoreType.DMA((2, 2))],
        compiler_params=pltpu.CompilerParams(vmem_limit_bytes=4 * 2**20),
        cost_estimate=pl.CostEstimate(flops=1_000_000, bytes_accessed=1_000_000, transcendentals=0),
    )(came, *parts)


def spread_kernel(part, first_ref, x_ref, o0_ref, o1_ref, o2_ref, o3_ref, sem):
    copies = [
        pltpu.make_async_copy(
            x_ref.at[pl.ds(first_ref[k], HALF), pl.ds(part * PART, PART)], out, sem.at[k]
        )
        for k, out in enumerate((o0_ref, o1_ref, o2_ref, o3_ref))
    ]
    for copy in copies:
        copy.start()
    for copy in copies:
        copy.wait()


def spread(part, first, tokens):
    out = jax.ShapeDtypeStruct((HALF, PART, WIDTH), jnp.bfloat16)
    return pl.pallas_call(
        functools.partial(spread_kernel, part),
        out_shape=(out,) * 4,
        in_specs=[pl.BlockSpec(memory_space=pltpu.SMEM), pl.BlockSpec(memory_space=pltpu.HBM)],
        out_specs=(pl.BlockSpec(memory_space=pltpu.VMEM),) * 4,
        scratch_shapes=[pltpu.SemaphoreType.DMA((4,))],
        compiler_params=pltpu.CompilerParams(vmem_limit_bytes=6 * 2**20),
        cost_estimate=pl.CostEstimate(flops=1_000_000, bytes_accessed=4_000_000, transcendentals=0),
    )(first, tokens)


def project_kernel(
    came_ref, head_ref, x0_ref, x1_ref, x2_ref, x3_ref, w_ref, mine_ref, send_ref, x, normal, sem,
):
    core = head_ref[2]
    for r in range(2):
        for k, ref in enumerate((x0_ref, x1_ref, x2_ref, x3_ref)):

            @pl.when(came_ref[r] == k)
            def _():
                for side, at in ((0, 2 * core), (1, 2 - 2 * core)):
                    pltpu.make_async_copy(
                        ref.at[pl.ds(at, 2)], x.at[side, pl.ds(2 * r, 2)], sem.at[r, side]
                    ).start()

    for side in (0, 1):
        side = 1 - side
        for r in range(2):
            pltpu.make_async_copy(
                x0_ref.at[pl.ds(0, 2)], x.at[side, pl.ds(2 * r, 2)], sem.at[r, side]
            ).wait()
        values = x[side].reshape(4 * PART, WIDTH).astype(jnp.float32)
        centred = values - jnp.mean(values, axis=-1, keepdims=True)
        variance = jnp.mean(centred * centred, axis=-1, keepdims=True)
        normal[side] = (centred * lax.rsqrt(variance + norm_eps)).astype(jnp.bfloat16)
    for n in range(8):
        cols = slice(n * 256, (n + 1) * 256)
        both = normal[...].reshape(8 * PART, WIDTH)
        out = jnp.dot(both, w_ref[:, cols], preferred_element_type=jnp.float32)
        out = (out * HEAD_DIM ** (-0.5)).astype(jnp.bfloat16).reshape(2, 4, PART, 256)
        mine_ref[:, :, cols] = out[0]
        send_ref[:, :, cols] = out[1]


def project(came, head, parts, w_query):
    smem = pl.BlockSpec(memory_space=pltpu.SMEM)
    vmem = pl.BlockSpec(memory_space=pltpu.VMEM)
    out = jax.ShapeDtypeStruct((4, PART, WIDTH), jnp.bfloat16)
    return pl.pallas_call(
        project_kernel,
        out_shape=(out, out),
        in_specs=[smem, smem] + [pl.BlockSpec(memory_space=pl.ANY)] * 4 + [vmem],
        out_specs=(vmem, vmem),
        scratch_shapes=[
            pltpu.VMEM((2, 4, PART, WIDTH), jnp.bfloat16),
            pltpu.VMEM((2, 4 * PART, WIDTH), jnp.bfloat16),
            pltpu.SemaphoreType.DMA((2, 2)),
        ],
        compiler_params=pltpu.CompilerParams(vmem_limit_bytes=16 * 2**20),
        cost_estimate=pl.CostEstimate(
            flops=2_150_000_000, bytes_accessed=12_000_000, transcendentals=0
        ),
    )(came, head, *parts, w_query)


def attend_kernel(
    rank, head_ref, qm0_ref, qm1_ref, qt0_ref, qt1_ref,
    own_ref, prev_ref, next_ref, opa_ref, opb_ref, w_ref, om_ref, ot_ref, ctx,
):
    z, y, core = head_ref[0], head_ref[1], head_ref[2]
    i = lax.broadcasted_iota(jnp.int32, (1, IMG), 1)
    run, which, within = i // 64, (i // 16) & 3, i & 15
    hop = jnp.where(run == 1, 3, jnp.where(run == 2, 1, jnp.where(run == 3, 2, 0)))
    back = 4 - which
    at_z = (z + jnp.where(core == 0, back, hop)) & 3
    at_y = (y + jnp.where(core == 0, hop, back)) & 3
    within = (within & 7) + 8 * jnp.where(within < 8, core, 1 - core)
    key_at = 64 * at_z + 16 * at_y + within
    for j in range(2):
        bias = jnp.where(key_at < head_ref[3 + j], 0.0, masked_score)
        for h in range(HEADS):
            cols = slice(h * HEAD_DIM, (h + 1) * HEAD_DIM)

            def side(kv):
                return jnp.concatenate(
                    [
                        ref[:, kv, j, :, cols].reshape(-1, HEAD_DIM)
                        for ref in (own_ref, prev_ref, next_ref, opa_ref, opb_ref)
                    ],
                    axis=0,
                )

            q = jnp.concatenate(
                [ref[2 * rank + j, :, cols] for ref in (qm0_ref, qm1_ref, qt0_ref, qt1_ref)],
                axis=0,
            )
            scores = lax.dot_general(
                q, side(0), (((1,), (1,)), ((), ())), preferred_element_type=jnp.float32
            )
            scores = scores + bias
            top = jnp.max(scores, axis=-1, keepdims=True)
            probs = jnp.exp(scores - top)
            total = jnp.sum(probs, axis=-1, keepdims=True)
            mixed = jnp.dot(
                probs.astype(jnp.bfloat16), side(1), preferred_element_type=jnp.float32
            )
            ctx[2 * ROWS * j : 2 * ROWS * (j + 1), cols] = (mixed * (1.0 / total)).astype(jnp.bfloat16)

    row = lax.broadcasted_iota(jnp.int32, (ROWS, 1), 0)
    for n in range(8):
        cols = slice(n * 256, (n + 1) * 256)
        out = jnp.dot(ctx[...], w_ref[:, cols], preferred_element_type=jnp.float32)
        for j in range(2):
            for side, ref in ((0, om_ref), (1, ot_ref)):
                at = (2 * j + side) * ROWS
                kept = row < head_ref[5 + 2 * j + side]
                ref[j, :, cols] = jnp.where(kept, out[at : at + ROWS], 0.0).astype(jnp.bfloat16)


def attend(rank, head, queries, pieces, w_out):
    vmem = pl.BlockSpec(memory_space=pltpu.VMEM)
    out = jax.ShapeDtypeStruct((2, ROWS, WIDTH), jnp.bfloat16)
    return pl.pallas_call(
        functools.partial(attend_kernel, rank),
        out_shape=(out, out),
        in_specs=[pl.BlockSpec(memory_space=pltpu.SMEM)] + [vmem] * 10,
        out_specs=(vmem, vmem),
        scratch_shapes=[pltpu.VMEM((4 * ROWS, WIDTH), jnp.bfloat16)],
        compiler_params=pltpu.CompilerParams(vmem_limit_bytes=20 * 2**20),
        cost_estimate=pl.CostEstimate(
            flops=3_500_000_000, bytes_accessed=14_000_000, transcendentals=1_000_000
        ),
    )(head, *queries, *pieces, w_out)


def place_kernel(index_ref, m0_ref, m1_ref, t0_ref, t1_ref, out_ref, zeros, sem):
    zeros[...] = jnp.zeros_like(zeros)
    for slot in range(SLOTS):
        source = index_ref[slot]
        for n, ref in enumerate((m0_ref, m1_ref, t0_ref, t1_ref)):
            for j in range(2):

                @pl.when(source == 2 * n + j)
                def _():
                    pltpu.make_async_copy(ref.at[j], out_ref.at[slot], sem.at[slot]).start()

        @pl.when(source < 0)
        def _():
            pltpu.make_async_copy(zeros, out_ref.at[slot], sem.at[slot]).start()

    for slot in range(SLOTS):
        pltpu.make_async_copy(zeros, out_ref.at[slot], sem.at[slot]).wait()


def place(index, m0, m1, t0, t1):
    return pl.pallas_call(
        place_kernel,
        out_shape=jax.ShapeDtypeStruct((SLOTS, ROWS, WIDTH), jnp.bfloat16),
        in_specs=[pl.BlockSpec(memory_space=pltpu.SMEM)]
        + [pl.BlockSpec(memory_space=pltpu.VMEM)] * 4,
        out_specs=pl.BlockSpec(memory_space=pl.ANY),
        scratch_shapes=[
            pltpu.VMEM((ROWS, WIDTH), jnp.bfloat16),
            pltpu.SemaphoreType.DMA((SLOTS,)),
        ],
        compiler_params=pltpu.CompilerParams(vmem_limit_bytes=8 * 2**20),
        cost_estimate=pl.CostEstimate(
            flops=1_000_000, bytes_accessed=4_000_000, transcendentals=0
        ),
    )(index, m0, m1, t0, t1)


def compute(
    tokens, image_keys, image_values, text_len, image_len, counts, old_group, new_group, w_query, w_out
):
    *kv, first, came, head0, head1, index = pack(
        counts, old_group, new_group, text_len, image_len, image_keys, image_values
    )

    for k in (1, 3, 2):
        kv[k] = move_group(kv[k], k)
    parts = []
    for part in range(2):
        x = list(spread(part, first, tokens))
        for k in (1, 3, 2):
            x[k] = move_group(x[k], k)
        parts.append(x)

    kv_mine, kv_send = choose(came, kv)
    kv_theirs = move_seq(kv_send, "swap")
    block = [jnp.concatenate([kv_mine[r], kv_theirs[r]], axis=2) for r in range(2)]

    pieces = []
    for r in range(2):
        near = [block[r]]
        for k in (1, 2, 3):
            near.append(move_seq(block[r], "near", k))
        own = jnp.stack(near)
        prev = move_seq(own, "far", 1)
        after = move_seq(own, "far", 3)
        opa = move_seq(prev[:2], "far", 1)
        opb = move_seq(after[2:], "far", 3)
        pieces.append((own, prev, after, opa, opb))

    mine, theirs = [], []
    for part in range(2):
        q_mine, q_send = project(came, head0, parts[part], w_query)
        mine.append(q_mine)
        theirs.append(move_seq(q_send, "swap"))

    done = []
    for r, head in enumerate((head0, head1)):
        out_mine, out_send = attend(r, head, mine + theirs, pieces[r], w_out)
        done.append((out_mine, move_seq(out_send, "swap")))
    return place(index, done[0][0], done[1][0], done[0][1], done[1][1])


def solution(mesh):
    split = P("group", "seq", None)
    return jax.shard_map(
        compute,
        mesh=mesh,
        in_specs=(split,) * 3 + (P(),) * 7,
        out_specs=split,
        check_vma=False,
    )
```

```python
import functools

import jax
import jax.numpy as jnp
from jax import lax
from jax.experimental import pallas as pl
from jax.experimental.pallas import tpu as pltpu
from jax.sharding import PartitionSpec as P


HEADS = 16
HEAD_DIM = 128
WIDTH = 2048
GROUPS = 4
SLOTS = 8
TASKS = 6
HALF = 4
RING = 4
CORES = 2
ROWS = 64
PART = 32
KEYS = 8
IMG = 256

masked_score = -1e30
norm_eps = 1e-05


def seq_moves(phase, k):
    pairs = []
    for z in range(RING):
        for y in range(RING):
            for c in range(CORES):
                z2, y2, c2 = z, y, c
                if phase == "swap":
                    c2 = 1 - c
                elif (phase == "near") == (c == 0):
                    z2 = (z + k) % RING
                else:
                    y2 = (y + k) % RING
                pairs.append(((z * RING + y) * CORES + c, (z2 * RING + y2) * CORES + c2))
    return pairs


def move_seq(a, phase, k=1):
    return lax.ppermute(a, "seq", seq_moves(phase, k))


def move_group(a, k):
    return lax.ppermute(a, "group", [(g, (g + k) % GROUPS) for g in range(GROUPS)])


def pack_kernel(
    counts_ref, old_ref, new_ref, text_ref, image_ref, k_ref, v_ref,
    kv0_ref, kv1_ref, kv2_ref, kv3_ref, first_ref, came_ref, head0_ref, head1_ref, index_ref, sem,
):
    group, d = lax.axis_index("group"), lax.axis_index("seq")
    core = d % CORES
    y = (d // CORES) % RING
    z = d // (CORES * RING)
    tasks = range(TASKS)
    count = [counts_ref[t] for t in tasks]
    old = [old_ref[t] for t in tasks]
    new = [new_ref[t] for t in tasks]
    zero = jnp.int32(0)
    start, rank = [], []
    for t in tasks:
        at, before = zero, zero
        for u in range(t):
            at = at + jnp.where(old[u] == old[t], count[u], 0)
            before = before + jnp.where(new[u] == new[t], 1, 0)
        start.append(at)
        rank.append(before)
    copies = []
    for k, out in enumerate((kv0_ref, kv1_ref, kv2_ref, kv3_ref)):
        first = zero
        for t in tasks:
            goes = (old[t] == group) & (new[t] == (group + k) % GROUPS)
            first = jnp.where(goes, start[t], first)
        first_ref[k] = first
        for i, ref in enumerate((k_ref, v_ref)):
            copies.append(
                pltpu.make_async_copy(ref.at[pl.ds(first, HALF)], out.at[i], sem.at[2 * k + i])
            )
            copies[-1].start()
    amounts = []
    for r, head in enumerate((head0_ref, head1_ref)):
        came, amount, base = zero, zero, zero
        for t in tasks:
            mine = (new[t] == group) & (rank[t] == r)
            came = jnp.where(mine, (group - old[t] + GROUPS) % GROUPS, came)
            amount = jnp.where(mine, count[t], amount)
            base = jnp.where(mine, old[t] * SLOTS + start[t], base)
        came_ref[r] = came
        amounts.append(amount)
        head[0], head[1], head[2] = z, y, core
        for j in range(2):
            sample = 2 * core + j
            there = sample < amount
            slot = jnp.where(there, base + sample, 0)
            head[3 + j] = jnp.where(there, image_ref[slot], IMG)
            text = jnp.where(there, text_ref[slot], 0)
            head[5 + 2 * j] = text - d * ROWS
            head[6 + 2 * j] = text - (d + 1 - 2 * core) * ROWS
    for slot in range(SLOTS):
        second = jnp.where(slot >= amounts[0], 1, 0)
        j = slot - second * amounts[0]
        at = jnp.where(j // 2 == core, 0, 4) + 2 * second + j % 2
        index_ref[slot] = jnp.where(slot < amounts[0] + amounts[1], at, -1)
    for copy in copies:
        copy.wait()


def pack(counts, old_group, new_group, text_len, image_len, keys, values):
    smem = pl.BlockSpec(memory_space=pltpu.SMEM)
    vmem = pl.BlockSpec(memory_space=pltpu.VMEM)
    kv = jax.ShapeDtypeStruct((2, HALF, KEYS, WIDTH), jnp.bfloat16)
    ints = [jax.ShapeDtypeStruct((n,), jnp.int32) for n in (4, 2, 9, 9, 8)]
    return pl.pallas_call(
        pack_kernel,
        out_shape=(kv,) * 4 + tuple(ints),
        in_specs=[smem] * 5 + [pl.BlockSpec(memory_space=pltpu.HBM)] * 2,
        out_specs=(vmem,) * 4 + (smem,) * 5,
        scratch_shapes=[pltpu.SemaphoreType.DMA((8,))],
        compiler_params=pltpu.CompilerParams(vmem_limit_bytes=6 * 2**20),
        cost_estimate=pl.CostEstimate(flops=1_000_000, bytes_accessed=2_000_000, transcendentals=0),
    )(counts, old_group, new_group, text_len, image_len, keys, values)


def choose_kernel(came_ref, kv0_ref, kv1_ref, kv2_ref, kv3_ref, mine_ref, send_ref, sem):
    core = lax.axis_index("seq") % CORES
    for r in range(2):
        for k, ref in enumerate((kv0_ref, kv1_ref, kv2_ref, kv3_ref)):

            @pl.when(came_ref[r] == k)
            def _():
                for side, (at, out) in enumerate(((2 * core, mine_ref), (2 - 2 * core, send_ref))):
                    pltpu.make_async_copy(
                        ref.at[:, pl.ds(at, 2)], out.at[r], sem.at[r, side]
                    ).start()

    for r in range(2):
        for side, out in enumerate((mine_ref, send_ref)):
            pltpu.make_async_copy(kv0_ref.at[:, pl.ds(0, 2)], out.at[r], sem.at[r, side]).wait()


def choose(came, parts):
    out = jax.ShapeDtypeStruct((2, 2, 2, KEYS, WIDTH), jnp.bfloat16)
    return pl.pallas_call(
        choose_kernel,
        out_shape=(out, out),
        in_specs=[pl.BlockSpec(memory_space=pltpu.SMEM)] + [pl.BlockSpec(memory_space=pl.ANY)] * 4,
        out_specs=(pl.BlockSpec(memory_space=pltpu.VMEM),) * 2,
        scratch_shapes=[pltpu.SemaphoreType.DMA((2, 2))],
        compiler_params=pltpu.CompilerParams(vmem_limit_bytes=4 * 2**20),
        cost_estimate=pl.CostEstimate(flops=1_000_000, bytes_accessed=1_000_000, transcendentals=0),
    )(came, *parts)


def scaled_queries(normal, w_ref, n):
    out = jnp.dot(normal, w_ref[:, n * 256 : (n + 1) * 256], preferred_element_type=jnp.float32)
    return (out * HEAD_DIM ** (-0.5)).astype(jnp.bfloat16)


def normalized(x):
    values = x.reshape(-1, WIDTH).astype(jnp.float32)
    centred = values - jnp.mean(values, axis=-1, keepdims=True)
    variance = jnp.mean(centred * centred, axis=-1, keepdims=True)
    return (centred * lax.rsqrt(variance + norm_eps)).astype(jnp.bfloat16)


def start_picks(came_ref, core, parts, mine, send, sem):
    for r in range(2):
        for k, ref in enumerate(parts):

            @pl.when(came_ref[r] == k)
            def _():
                for side, (at, out) in enumerate(((2 * core, mine), (2 - 2 * core, send))):
                    pltpu.make_async_copy(
                        ref.at[pl.ds(at, 2)], out.at[pl.ds(2 * r, 2)], sem.at[r, side]
                    ).start()


def wait_picks(parts, side, out, sem):
    for r in range(2):
        pltpu.make_async_copy(
            parts[0].at[pl.ds(0, 2)], out.at[pl.ds(2 * r, 2)], sem.at[r, side]
        ).wait()


def project_kernel(
    came_ref, head_ref, x0_ref, x1_ref, x2_ref, x3_ref, w_ref, mine_ref, send_ref, x, normal, sem,
):
    parts = (x0_ref, x1_ref, x2_ref, x3_ref)
    start_picks(came_ref, head_ref[2], parts, x.at[0], x.at[1], sem)
    for side in range(2):
        wait_picks(parts, side, x.at[side], sem)
        normal[side] = normalized(x[side])
    for n in range(8):
        both = normal[...].reshape(8 * PART, WIDTH)
        out = scaled_queries(both, w_ref, n).reshape(2, 4, PART, 256)
        mine_ref[:, :, n * 256 : (n + 1) * 256] = out[0]
        send_ref[:, :, n * 256 : (n + 1) * 256] = out[1]


def project(came, head, parts, w_query):
    smem = pl.BlockSpec(memory_space=pltpu.SMEM)
    vmem = pl.BlockSpec(memory_space=pltpu.VMEM)
    out = jax.ShapeDtypeStruct((4, PART, WIDTH), jnp.bfloat16)
    return pl.pallas_call(
        project_kernel,
        out_shape=(out, out),
        in_specs=[smem, smem] + [pl.BlockSpec(memory_space=pl.ANY)] * 4 + [vmem],
        out_specs=(vmem, vmem),
        scratch_shapes=[
            pltpu.VMEM((2, 4, PART, WIDTH), jnp.bfloat16),
            pltpu.VMEM((2, 4 * PART, WIDTH), jnp.bfloat16),
            pltpu.SemaphoreType.DMA((2, 2)),
        ],
        compiler_params=pltpu.CompilerParams(vmem_limit_bytes=16 * 2**20),
        cost_estimate=pl.CostEstimate(
            flops=2_150_000_000, bytes_accessed=12_000_000, transcendentals=0
        ),
    )(came, head, *parts, w_query)


def early_kernel(
    first_ref, x_ref, w_hbm, t0_ref, t1_ref, t2_ref, t3_ref, o0_ref, o1_ref, o2_ref, o3_ref,
    x, normal, queries, w_ref, sem, w_sem, t_sem,
):
    raw = [
        pltpu.make_async_copy(
            x_ref.at[pl.ds(first_ref[k], HALF), pl.ds(0, PART)], out, t_sem.at[k]
        )
        for k, out in enumerate((t0_ref, t1_ref, t2_ref, t3_ref))
    ]
    blocks = [
        pltpu.make_async_copy(
            w_hbm.at[:, pl.ds(512 * i, 512)], w_ref.at[:, pl.ds(512 * i, 512)], w_sem.at[i]
        )
        for i in range(4)
    ]
    copies = [
        pltpu.make_async_copy(
            x_ref.at[pl.ds(4 * i, 4), pl.ds(PART, PART)], x.at[pl.ds(4 * i, 4)], sem.at[i]
        )
        for i in range(2)
    ]
    for copy in copies + blocks + raw:
        copy.start()
    for i, copy in enumerate(copies):
        copy.wait()
        normal[4 * PART * i : 4 * PART * (i + 1)] = normalized(x[4 * i : 4 * i + 4])
    for n in range(8):
        if n % 2 == 0:
            blocks[n // 2].wait()
        out = scaled_queries(normal[...], w_ref, n)
        queries[:, :, n * 256 : (n + 1) * 256] = out.reshape(SLOTS, PART, 256)
    for k, out in enumerate((o0_ref, o1_ref, o2_ref, o3_ref)):
        out[...] = queries[pl.ds(first_ref[k], HALF)]
    for copy in raw:
        copy.wait()


def early(first, tokens, w_query):
    vmem = pl.BlockSpec(memory_space=pltpu.VMEM)
    out = jax.ShapeDtypeStruct((HALF, PART, WIDTH), jnp.bfloat16)
    return pl.pallas_call(
        early_kernel,
        out_shape=(out,) * 8,
        in_specs=[
            pl.BlockSpec(memory_space=pltpu.SMEM),
            pl.BlockSpec(memory_space=pltpu.HBM),
            pl.BlockSpec(memory_space=pltpu.HBM),
        ],
        out_specs=(vmem,) * 8,
        scratch_shapes=[
            pltpu.VMEM((SLOTS, PART, WIDTH), jnp.bfloat16),
            pltpu.VMEM((SLOTS * PART, WIDTH), jnp.bfloat16),
            pltpu.VMEM((SLOTS, PART, WIDTH), jnp.bfloat16),
            pltpu.VMEM((WIDTH, WIDTH), jnp.bfloat16),
            pltpu.SemaphoreType.DMA((2,)),
            pltpu.SemaphoreType.DMA((4,)),
            pltpu.SemaphoreType.DMA((4,)),
        ],
        compiler_params=pltpu.CompilerParams(vmem_limit_bytes=20 * 2**20),
        cost_estimate=pl.CostEstimate(
            flops=2_150_000_000, bytes_accessed=12_000_000, transcendentals=0
        ),
    )(first, tokens, w_query)


def late_kernel(came_ref, head_ref, x0_ref, x1_ref, x2_ref, x3_ref, mine_ref, send_ref, sem):
    parts = (x0_ref, x1_ref, x2_ref, x3_ref)
    start_picks(came_ref, head_ref[2], parts, mine_ref, send_ref, sem)
    wait_picks(parts, 0, mine_ref, sem)
    wait_picks(parts, 1, send_ref, sem)


def late(came, head, parts):
    smem = pl.BlockSpec(memory_space=pltpu.SMEM)
    vmem = pl.BlockSpec(memory_space=pltpu.VMEM)
    out = jax.ShapeDtypeStruct((4, PART, WIDTH), jnp.bfloat16)
    return pl.pallas_call(
        late_kernel,
        out_shape=(out, out),
        in_specs=[smem, smem] + [pl.BlockSpec(memory_space=pl.ANY)] * 4,
        out_specs=(vmem, vmem),
        scratch_shapes=[pltpu.SemaphoreType.DMA((2, 2))],
        compiler_params=pltpu.CompilerParams(vmem_limit_bytes=4 * 2**20),
        cost_estimate=pl.CostEstimate(flops=1_000_000, bytes_accessed=2_000_000, transcendentals=0),
    )(came, head, *parts)


def attend_kernel(
    rank, head_ref, qm0_ref, qm1_ref, qt0_ref, qt1_ref,
    own_ref, prev_ref, next_ref, opa_ref, opb_ref, w_ref, om_ref, ot_ref, ctx,
):
    z, y, core = head_ref[0], head_ref[1], head_ref[2]
    i = lax.broadcasted_iota(jnp.int32, (1, IMG), 1)
    run, which, within = i // 64, (i // 16) & 3, i & 15
    hop = jnp.where(run == 1, 3, jnp.where(run == 2, 1, jnp.where(run == 3, 2, 0)))
    back = 4 - which
    at_z = (z + jnp.where(core == 0, back, hop)) & 3
    at_y = (y + jnp.where(core == 0, hop, back)) & 3
    within = (within & 7) + 8 * jnp.where(within < 8, core, 1 - core)
    key_at = 64 * at_z + 16 * at_y + within
    for j in range(2):
        bias = jnp.where(key_at < head_ref[3 + j], 0.0, masked_score)
        for h in range(HEADS):
            cols = slice(h * HEAD_DIM, (h + 1) * HEAD_DIM)

            def side(kv):
                return jnp.concatenate(
                    [
                        ref[:, kv, j, :, cols].reshape(-1, HEAD_DIM)
                        for ref in (own_ref, prev_ref, next_ref, opa_ref, opb_ref)
                    ],
                    axis=0,
                )

            q = jnp.concatenate(
                [ref[2 * rank + j, :, cols] for ref in (qm0_ref, qm1_ref, qt0_ref, qt1_ref)],
                axis=0,
            )
            scores = lax.dot_general(
                q, side(0), (((1,), (1,)), ((), ())), preferred_element_type=jnp.float32
            )
            scores = scores + bias
            top = jnp.max(scores, axis=-1, keepdims=True)
            probs = jnp.exp(scores - top)
            total = jnp.sum(probs, axis=-1, keepdims=True)
            mixed = jnp.dot(
                probs.astype(jnp.bfloat16), side(1), preferred_element_type=jnp.float32
            )
            ctx[2 * ROWS * j : 2 * ROWS * (j + 1), cols] = (mixed * (1.0 / total)).astype(jnp.bfloat16)

    row = lax.broadcasted_iota(jnp.int32, (ROWS, 1), 0)
    for n in range(8):
        cols = slice(n * 256, (n + 1) * 256)
        out = jnp.dot(ctx[...], w_ref[:, cols], preferred_element_type=jnp.float32)
        for j in range(2):
            for side, ref in ((0, om_ref), (1, ot_ref)):
                at = (2 * j + side) * ROWS
                kept = row < head_ref[5 + 2 * j + side]
                ref[j, :, cols] = jnp.where(kept, out[at : at + ROWS], 0.0).astype(jnp.bfloat16)


def attend(rank, head, queries, pieces, w_out):
    vmem = pl.BlockSpec(memory_space=pltpu.VMEM)
    out = jax.ShapeDtypeStruct((2, ROWS, WIDTH), jnp.bfloat16)
    return pl.pallas_call(
        functools.partial(attend_kernel, rank),
        out_shape=(out, out),
        in_specs=[pl.BlockSpec(memory_space=pltpu.SMEM)] + [vmem] * 10,
        out_specs=(vmem, vmem),
        scratch_shapes=[pltpu.VMEM((4 * ROWS, WIDTH), jnp.bfloat16)],
        compiler_params=pltpu.CompilerParams(vmem_limit_bytes=20 * 2**20),
        cost_estimate=pl.CostEstimate(
            flops=3_500_000_000, bytes_accessed=14_000_000, transcendentals=1_000_000
        ),
    )(head, *queries, *pieces, w_out)


def place_kernel(index_ref, m0_ref, m1_ref, t0_ref, t1_ref, out_ref, zeros, sem):
    zeros[...] = jnp.zeros_like(zeros)
    for slot in range(SLOTS):
        source = index_ref[slot]
        for n, ref in enumerate((m0_ref, m1_ref, t0_ref, t1_ref)):
            for j in range(2):

                @pl.when(source == 2 * n + j)
                def _():
                    pltpu.make_async_copy(ref.at[j], out_ref.at[slot], sem.at[slot]).start()

        @pl.when(source < 0)
        def _():
            pltpu.make_async_copy(zeros, out_ref.at[slot], sem.at[slot]).start()

    for slot in range(SLOTS):
        pltpu.make_async_copy(zeros, out_ref.at[slot], sem.at[slot]).wait()


def place(index, m0, m1, t0, t1):
    return pl.pallas_call(
        place_kernel,
        out_shape=jax.ShapeDtypeStruct((SLOTS, ROWS, WIDTH), jnp.bfloat16),
        in_specs=[pl.BlockSpec(memory_space=pltpu.SMEM)]
        + [pl.BlockSpec(memory_space=pltpu.VMEM)] * 4,
        out_specs=pl.BlockSpec(memory_space=pl.ANY),
        scratch_shapes=[
            pltpu.VMEM((ROWS, WIDTH), jnp.bfloat16),
            pltpu.SemaphoreType.DMA((SLOTS,)),
        ],
        compiler_params=pltpu.CompilerParams(vmem_limit_bytes=8 * 2**20),
        cost_estimate=pl.CostEstimate(
            flops=1_000_000, bytes_accessed=4_000_000, transcendentals=0
        ),
    )(index, m0, m1, t0, t1)


def compute(
    tokens, image_keys, image_values, text_len, image_len, counts, old_group, new_group, w_query, w_out
):
    small = (counts, old_group, new_group, text_len, image_len, image_keys, image_values, tokens)
    counts, old_group, new_group, text_len, image_len, image_keys, image_values, tokens = (
        pltpu.with_memory_space_constraint(a, pltpu.HBM) for a in small
    )
    w_far = pltpu.with_memory_space_constraint(w_query, pltpu.HBM)
    *kv, first, came, head0, head1, index = pack(
        counts, old_group, new_group, text_len, image_len, image_keys, image_values
    )

    for k in (1, 3, 2):
        kv[k] = move_group(kv[k], k)
    parts = []
    ready = early(first, tokens, w_far)
    for part in range(2):
        x = list(ready[4 * part : 4 * part + 4])
        for k in (1, 3, 2):
            x[k] = move_group(x[k], k)
        parts.append(x)

    kv_mine, kv_send = choose(came, kv)
    kv_theirs = move_seq(kv_send, "swap")
    block = [jnp.concatenate([kv_mine[r], kv_theirs[r]], axis=2) for r in range(2)]

    pieces = []
    for r in range(2):
        near = [block[r]]
        for k in (1, 2, 3):
            near.append(move_seq(block[r], "near", k))
        own = jnp.stack(near)
        prev = move_seq(own, "far", 1)
        after = move_seq(own, "far", 3)
        opa = move_seq(prev[:2], "far", 1)
        opb = move_seq(after[2:], "far", 3)
        pieces.append((own, prev, after, opa, opb))

    mine, theirs = [], []
    for part in range(2):
        if part:
            q_mine, q_send = late(came, head0, parts[1])
        else:
            q_mine, q_send = project(came, head0, parts[0], w_query)
        mine.append(q_mine)
        theirs.append(move_seq(q_send, "swap"))

    done = []
    for r, head in enumerate((head0, head1)):
        out_mine, out_send = attend(r, head, mine + theirs, pieces[r], w_out)
        done.append((out_mine, move_seq(out_send, "swap")))
    return place(index, done[0][0], done[1][0], done[0][1], done[1][1])


def solution(mesh):
    split = P("group", "seq", None)
    return jax.shard_map(
        compute,
        mesh=mesh,
        in_specs=(split,) * 3 + (P(),) * 7,
        out_specs=split,
        check_vma=False,
    )
```

```python
import functools

import jax
import jax.numpy as jnp
from jax import lax
from jax.experimental import pallas as pl
from jax.experimental.pallas import tpu as pltpu
from jax.sharding import PartitionSpec as P


HEADS = 16
HEAD_DIM = 128
WIDTH = 2048
GROUPS = 4
SLOTS = 8
TASKS = 6
HALF = 4
RING = 4
CORES = 2
ROWS = 64
KEYS = 8
IMG = 256

masked_score = -1e30
norm_eps = 1e-05


def seq_moves(phase, k):
    pairs = []
    for z in range(RING):
        for y in range(RING):
            for c in range(CORES):
                z2, y2, c2 = z, y, c
                if phase == "swap":
                    c2 = 1 - c
                elif (phase == "near") == (c == 0):
                    z2 = (z + k) % RING
                else:
                    y2 = (y + k) % RING
                pairs.append(((z * RING + y) * CORES + c, (z2 * RING + y2) * CORES + c2))
    return pairs


def move_seq(a, phase, k=1):
    return lax.ppermute(a, "seq", seq_moves(phase, k))


def move_group(a, k):
    return lax.ppermute(a, "group", [(g, (g + k) % GROUPS) for g in range(GROUPS)])


def pack_kernel(
    counts_hbm, old_hbm, new_hbm, text_hbm, image_hbm, k_ref, v_ref,
    kv0_ref, kv1_ref, kv2_ref, kv3_ref, first_ref, came_ref, head0_ref, head1_ref, index_ref,
    counts_ref, old_ref, new_ref, text_ref, image_ref, sem, int_sem,
):
    ints = [
        pltpu.make_async_copy(source, ref, int_sem.at[i])
        for i, (source, ref) in enumerate(
            (
                (counts_hbm, counts_ref),
                (old_hbm, old_ref),
                (new_hbm, new_ref),
                (text_hbm, text_ref),
                (image_hbm, image_ref),
            )
        )
    ]
    for copy in ints:
        copy.start()
    for copy in ints[:3]:
        copy.wait()
    group, d = lax.axis_index("group"), lax.axis_index("seq")
    core = d % CORES
    y = (d // CORES) % RING
    z = d // (CORES * RING)
    tasks = range(TASKS)
    count = [counts_ref[t] for t in tasks]
    old = [old_ref[t] for t in tasks]
    new = [new_ref[t] for t in tasks]
    zero = jnp.int32(0)
    start, rank = [], []
    for t in tasks:
        at, before = zero, zero
        for u in range(t):
            at = at + jnp.where(old[u] == old[t], count[u], 0)
            before = before + jnp.where(new[u] == new[t], 1, 0)
        start.append(at)
        rank.append(before)
    copies = []
    for k, out in enumerate((kv0_ref, kv1_ref, kv2_ref, kv3_ref)):
        first = zero
        for t in tasks:
            goes = (old[t] == group) & (new[t] == (group + k) % GROUPS)
            first = jnp.where(goes, start[t], first)
        first_ref[k] = first
        for i, ref in enumerate((k_ref, v_ref)):
            copies.append(
                pltpu.make_async_copy(ref.at[pl.ds(first, HALF)], out.at[i], sem.at[2 * k + i])
            )
            copies[-1].start()
    heads = (head0_ref, head1_ref)
    for head in heads:
        head[0], head[1], head[2] = z, y, core
    for copy in ints[3:]:
        copy.wait()
    amounts = []
    for r in range(2):
        came, amount, base = zero, zero, zero
        for t in tasks:
            mine = (new[t] == group) & (rank[t] == r)
            came = jnp.where(mine, (group - old[t] + GROUPS) % GROUPS, came)
            amount = jnp.where(mine, count[t], amount)
            base = jnp.where(mine, old[t] * SLOTS + start[t], base)
        came_ref[r] = came
        amounts.append(amount)
        for j, head in enumerate(heads):
            sample = 2 * core + j
            there = sample < amount
            slot = jnp.where(there, base + sample, 0)
            head[3 + r] = jnp.where(there, image_ref[slot], IMG)
            text = jnp.where(there, text_ref[slot], 0)
            head[5 + 2 * r] = text - d * ROWS
            head[6 + 2 * r] = text - (d + 1 - 2 * core) * ROWS
    for slot in range(SLOTS):
        second = jnp.where(slot >= amounts[0], 1, 0)
        j = slot - second * amounts[0]
        at = jnp.where(j // 2 == core, 0, 4) + 2 * (j % 2) + second
        index_ref[slot] = jnp.where(slot < amounts[0] + amounts[1], at, -1)
    for copy in copies:
        copy.wait()


def pack(counts, old_group, new_group, text_len, image_len, keys, values):
    smem = pl.BlockSpec(memory_space=pltpu.SMEM)
    vmem = pl.BlockSpec(memory_space=pltpu.VMEM)
    kv = jax.ShapeDtypeStruct((2, HALF, KEYS, WIDTH), jnp.bfloat16)
    ints = [jax.ShapeDtypeStruct((n,), jnp.int32) for n in (4, 2, 9, 9, 8)]
    numbers = (counts, old_group, new_group, text_len, image_len)
    return pl.pallas_call(
        pack_kernel,
        out_shape=(kv,) * 4 + tuple(ints),
        in_specs=[pl.BlockSpec(memory_space=pltpu.HBM)] * 7,
        out_specs=(vmem,) * 4 + (smem,) * 5,
        scratch_shapes=[pltpu.SMEM(a.shape, jnp.int32) for a in numbers]
        + [pltpu.SemaphoreType.DMA((8,)), pltpu.SemaphoreType.DMA((5,))],
        compiler_params=pltpu.CompilerParams(vmem_limit_bytes=6 * 2**20),
        cost_estimate=pl.CostEstimate(flops=1_000_000, bytes_accessed=2_000_000, transcendentals=0),
    )(*numbers, keys, values)


def choose_kernel(came_ref, kv0_ref, kv1_ref, kv2_ref, kv3_ref, mine_ref, send_ref, sem):
    core = lax.axis_index("seq") % CORES
    for r in range(2):
        for k, ref in enumerate((kv0_ref, kv1_ref, kv2_ref, kv3_ref)):

            @pl.when(came_ref[r] == k)
            def _():
                for j in range(2):
                    for side, (at, out) in enumerate(((core, mine_ref), (1 - core, send_ref))):
                        pltpu.make_async_copy(
                            ref.at[:, 2 * at + j], out.at[j, r], sem.at[r, j, side]
                        ).start()

    for r in range(2):
        for j in range(2):
            for side, out in enumerate((mine_ref, send_ref)):
                pltpu.make_async_copy(kv0_ref.at[:, 0], out.at[j, r], sem.at[r, j, side]).wait()


def choose(came, parts):
    out = jax.ShapeDtypeStruct((2, 2, 2, KEYS, WIDTH), jnp.bfloat16)
    return pl.pallas_call(
        choose_kernel,
        out_shape=(out, out),
        in_specs=[pl.BlockSpec(memory_space=pltpu.SMEM)] + [pl.BlockSpec(memory_space=pl.ANY)] * 4,
        out_specs=(pl.BlockSpec(memory_space=pltpu.VMEM),) * 2,
        scratch_shapes=[pltpu.SemaphoreType.DMA((2, 2, 2))],
        compiler_params=pltpu.CompilerParams(vmem_limit_bytes=4 * 2**20),
        cost_estimate=pl.CostEstimate(flops=1_000_000, bytes_accessed=1_000_000, transcendentals=0),
    )(came, *parts)


def scaled_queries(normal, w_ref, n):
    out = jnp.dot(normal, w_ref[:, n * 256 : (n + 1) * 256], preferred_element_type=jnp.float32)
    return (out * HEAD_DIM ** (-0.5)).astype(jnp.bfloat16)


def normalized(x):
    values = x.reshape(-1, WIDTH).astype(jnp.float32)
    centred = values - jnp.mean(values, axis=-1, keepdims=True)
    variance = jnp.mean(centred * centred, axis=-1, keepdims=True)
    return (centred * lax.rsqrt(variance + norm_eps)).astype(jnp.bfloat16)


def start_picks(came_ref, core, parts, mine, send, sem):
    for r in range(2):
        for k, ref in enumerate(parts):

            @pl.when(came_ref[r] == k)
            def _():
                for side, (at, out) in enumerate(((core, mine), (1 - core, send))):
                    pltpu.make_async_copy(ref.at[at], out.at[r], sem.at[r, side]).start()


def wait_picks(parts, side, out, sem):
    for r in range(2):
        pltpu.make_async_copy(parts[0].at[0], out.at[r], sem.at[r, side]).wait()


def project_kernel(
    came_ref, head_ref, x0_ref, x1_ref, x2_ref, x3_ref, w_ref, mine_ref, send_ref, x, normal, sem,
):
    parts = (x0_ref, x1_ref, x2_ref, x3_ref)
    start_picks(came_ref, head_ref[2], parts, x.at[0], x.at[1], sem)
    for side in range(2):
        wait_picks(parts, side, x.at[side], sem)
        normal[side] = normalized(x[side])
    for n in range(8):
        both = normal[...].reshape(4 * ROWS, WIDTH)
        out = scaled_queries(both, w_ref, n).reshape(2, 2, ROWS, 256)
        mine_ref[:, :, n * 256 : (n + 1) * 256] = out[0]
        send_ref[:, :, n * 256 : (n + 1) * 256] = out[1]


def project(came, head, parts, w_query):
    smem = pl.BlockSpec(memory_space=pltpu.SMEM)
    vmem = pl.BlockSpec(memory_space=pltpu.VMEM)
    out = jax.ShapeDtypeStruct((2, ROWS, WIDTH), jnp.bfloat16)
    return pl.pallas_call(
        project_kernel,
        out_shape=(out, out),
        in_specs=[smem, smem] + [pl.BlockSpec(memory_space=pl.ANY)] * 4 + [vmem],
        out_specs=(vmem, vmem),
        scratch_shapes=[
            pltpu.VMEM((2, 2, ROWS, WIDTH), jnp.bfloat16),
            pltpu.VMEM((2, 2 * ROWS, WIDTH), jnp.bfloat16),
            pltpu.SemaphoreType.DMA((2, 2)),
        ],
        compiler_params=pltpu.CompilerParams(vmem_limit_bytes=16 * 2**20),
        cost_estimate=pl.CostEstimate(
            flops=2_150_000_000, bytes_accessed=12_000_000, transcendentals=0
        ),
    )(came, head, *parts, w_query)


def early_kernel(
    first_ref, x_ref, w_hbm, t0_ref, t1_ref, t2_ref, t3_ref, o0_ref, o1_ref, o2_ref, o3_ref,
    x, normal, queries, w_ref, sem, w_sem, t_sem,
):
    second = jnp.int32(0)
    for k in range(GROUPS):
        second = jnp.maximum(second, first_ref[k])
    copies = [
        pltpu.make_async_copy(x_ref.at[at], x.at[i], sem.at[i])
        for i, at in enumerate((1, 3, second + 1, second + 3))
    ]
    blocks = [
        pltpu.make_async_copy(
            w_hbm.at[:, pl.ds(512 * i, 512)], w_ref.at[:, pl.ds(512 * i, 512)], w_sem.at[i]
        )
        for i in range(4)
    ]
    raw = [
        pltpu.make_async_copy(x_ref.at[first_ref[k] + 2 * i], out.at[i], t_sem.at[k, i])
        for k, out in enumerate((t0_ref, t1_ref, t2_ref, t3_ref))
        for i in range(2)
    ]
    for copy in copies + blocks[:2]:
        copy.start()
    for i in range(2):
        copies[2 * i].wait()
        copies[2 * i + 1].wait()
        blocks[2 + i].start()
        normal[2 * ROWS * i : 2 * ROWS * (i + 1)] = normalized(x[2 * i : 2 * i + 2])
    for copy in raw:
        copy.start()
    for n in range(8):
        if n % 2 == 0:
            blocks[n // 2].wait()
        out = scaled_queries(normal[...], w_ref, n)
        queries[:, :, n * 256 : (n + 1) * 256] = out.reshape(4, ROWS, 256)
    for k, out in enumerate((o0_ref, o1_ref, o2_ref, o3_ref)):
        out[...] = queries[pl.ds(jnp.where(first_ref[k] > 0, 2, 0), 2)]
    for copy in raw:
        copy.wait()


def early(first, tokens, w_query):
    vmem = pl.BlockSpec(memory_space=pltpu.VMEM)
    out = jax.ShapeDtypeStruct((2, ROWS, WIDTH), jnp.bfloat16)
    return pl.pallas_call(
        early_kernel,
        out_shape=(out,) * 8,
        in_specs=[
            pl.BlockSpec(memory_space=pltpu.SMEM),
            pl.BlockSpec(memory_space=pltpu.HBM),
            pl.BlockSpec(memory_space=pltpu.HBM),
        ],
        out_specs=(vmem,) * 8,
        scratch_shapes=[
            pltpu.VMEM((4, ROWS, WIDTH), jnp.bfloat16),
            pltpu.VMEM((4 * ROWS, WIDTH), jnp.bfloat16),
            pltpu.VMEM((4, ROWS, WIDTH), jnp.bfloat16),
            pltpu.VMEM((WIDTH, WIDTH), jnp.bfloat16),
            pltpu.SemaphoreType.DMA((4,)),
            pltpu.SemaphoreType.DMA((4,)),
            pltpu.SemaphoreType.DMA((4, 2)),
        ],
        compiler_params=pltpu.CompilerParams(vmem_limit_bytes=20 * 2**20),
        cost_estimate=pl.CostEstimate(
            flops=2_150_000_000, bytes_accessed=12_000_000, transcendentals=0
        ),
    )(first, tokens, w_query)


def late_kernel(came_ref, head_ref, x0_ref, x1_ref, x2_ref, x3_ref, mine_ref, send_ref, sem):
    parts = (x0_ref, x1_ref, x2_ref, x3_ref)
    start_picks(came_ref, head_ref[2], parts, mine_ref, send_ref, sem)
    wait_picks(parts, 0, mine_ref, sem)
    wait_picks(parts, 1, send_ref, sem)


def late(came, head, parts):
    smem = pl.BlockSpec(memory_space=pltpu.SMEM)
    vmem = pl.BlockSpec(memory_space=pltpu.VMEM)
    out = jax.ShapeDtypeStruct((2, ROWS, WIDTH), jnp.bfloat16)
    return pl.pallas_call(
        late_kernel,
        out_shape=(out, out),
        in_specs=[smem, smem] + [pl.BlockSpec(memory_space=pl.ANY)] * 4,
        out_specs=(vmem, vmem),
        scratch_shapes=[pltpu.SemaphoreType.DMA((2, 2))],
        compiler_params=pltpu.CompilerParams(vmem_limit_bytes=4 * 2**20),
        cost_estimate=pl.CostEstimate(flops=1_000_000, bytes_accessed=2_000_000, transcendentals=0),
    )(came, head, *parts)


def attend_kernel(
    head_ref, qm_ref, qt_ref, own_ref, prev_ref, next_ref, opa_ref, opb_ref, w_ref,
    om_ref, ot_ref, ctx,
):
    z, y, core = head_ref[0], head_ref[1], head_ref[2]
    i = lax.broadcasted_iota(jnp.int32, (1, IMG), 1)
    run, which, within = i // 64, (i // 16) & 3, i & 15
    hop = jnp.where(run == 1, 3, jnp.where(run == 2, 1, jnp.where(run == 3, 2, 0)))
    back = 4 - which
    at_z = (z + jnp.where(core == 0, back, hop)) & 3
    at_y = (y + jnp.where(core == 0, hop, back)) & 3
    within = (within & 7) + 8 * jnp.where(within < 8, core, 1 - core)
    key_at = 64 * at_z + 16 * at_y + within
    for r in range(2):
        bias = jnp.where(key_at < head_ref[3 + r], 0.0, masked_score)
        for h in range(HEADS):
            cols = slice(h * HEAD_DIM, (h + 1) * HEAD_DIM)

            def side(kv):
                return jnp.concatenate(
                    [
                        ref[:, r, kv, :, cols].reshape(-1, HEAD_DIM)
                        for ref in (own_ref, prev_ref, next_ref, opa_ref, opb_ref)
                    ],
                    axis=0,
                )

            q = jnp.concatenate([qm_ref[r, :, cols], qt_ref[r, :, cols]], axis=0)
            scores = lax.dot_general(
                q, side(0), (((1,), (1,)), ((), ())), preferred_element_type=jnp.float32
            )
            scores = scores + bias
            top = jnp.max(scores, axis=-1, keepdims=True)
            probs = jnp.exp(scores - top)
            total = jnp.sum(probs, axis=-1, keepdims=True)
            mixed = jnp.dot(
                probs.astype(jnp.bfloat16), side(1), preferred_element_type=jnp.float32
            )
            ctx[2 * ROWS * r : 2 * ROWS * (r + 1), cols] = (mixed * (1.0 / total)).astype(jnp.bfloat16)

    row = lax.broadcasted_iota(jnp.int32, (ROWS, 1), 0)
    for n in range(8):
        cols = slice(n * 256, (n + 1) * 256)
        out = jnp.dot(ctx[...], w_ref[:, cols], preferred_element_type=jnp.float32)
        for r in range(2):
            for side, ref in ((0, om_ref), (1, ot_ref)):
                at = (2 * r + side) * ROWS
                kept = row < head_ref[5 + 2 * r + side]
                ref[r, :, cols] = jnp.where(kept, out[at : at + ROWS], 0.0).astype(jnp.bfloat16)


def attend(head, queries, pieces, w_out):
    vmem = pl.BlockSpec(memory_space=pltpu.VMEM)
    out = jax.ShapeDtypeStruct((2, ROWS, WIDTH), jnp.bfloat16)
    return pl.pallas_call(
        attend_kernel,
        out_shape=(out, out),
        in_specs=[pl.BlockSpec(memory_space=pltpu.SMEM)] + [vmem] * 8,
        out_specs=(vmem, vmem),
        scratch_shapes=[pltpu.VMEM((4 * ROWS, WIDTH), jnp.bfloat16)],
        compiler_params=pltpu.CompilerParams(vmem_limit_bytes=20 * 2**20),
        cost_estimate=pl.CostEstimate(
            flops=3_500_000_000, bytes_accessed=14_000_000, transcendentals=1_000_000
        ),
    )(head, *queries, *pieces, w_out)


def place_kernel(at_first, index_ref, *refs):
    sources, (out_ref, zeros, sem) = refs[:-3], refs[-3:]
    if at_first == 0:
        zeros[...] = jnp.zeros_like(zeros)
    count = 2 * len(sources)
    for wait in (False, True):
        for slot in range(SLOTS):
            source = index_ref[slot] - at_first
            here = (source >= 0) & (source < count)
            if wait:
                copy = pltpu.make_async_copy(zeros, out_ref.at[slot], sem.at[slot])
                pl.when(here | (source < 0) if at_first == 0 else here)(copy.wait)
                continue
            for n, ref in enumerate(sources):
                for j in range(2):
                    copy = pltpu.make_async_copy(ref.at[j], out_ref.at[slot], sem.at[slot])
                    pl.when(source == 2 * n + j)(copy.start)
            if at_first == 0:
                copy = pltpu.make_async_copy(zeros, out_ref.at[slot], sem.at[slot])
                pl.when(source < 0)(copy.start)


def place_early(index, *sources):
    return pl.pallas_call(
        functools.partial(place_kernel, 0),
        out_shape=jax.ShapeDtypeStruct((SLOTS, ROWS, WIDTH), jnp.bfloat16),
        in_specs=[pl.BlockSpec(memory_space=pltpu.SMEM)]
        + [pl.BlockSpec(memory_space=pltpu.VMEM)] * 3,
        out_specs=pl.BlockSpec(memory_space=pltpu.HBM),
        scratch_shapes=[
            pltpu.VMEM((ROWS, WIDTH), jnp.bfloat16),
            pltpu.SemaphoreType.DMA((SLOTS,)),
        ],
        compiler_params=pltpu.CompilerParams(vmem_limit_bytes=8 * 2**20),
        cost_estimate=pl.CostEstimate(
            flops=1_000_000, bytes_accessed=3_000_000, transcendentals=0
        ),
    )(index, *sources)


def place_late_kernel(index_ref, source_ref, kept_ref, out_ref, zeros, sem):
    place_kernel(6, index_ref, source_ref, out_ref, zeros, sem)


def place_late(index, source, placed):
    hbm = pl.BlockSpec(memory_space=pltpu.HBM)
    return pl.pallas_call(
        place_late_kernel,
        out_shape=jax.ShapeDtypeStruct((SLOTS, ROWS, WIDTH), jnp.bfloat16),
        in_specs=[
            pl.BlockSpec(memory_space=pltpu.SMEM), pl.BlockSpec(memory_space=pltpu.VMEM), hbm
        ],
        out_specs=hbm,
        input_output_aliases={2: 0},
        scratch_shapes=[
            pltpu.VMEM((ROWS, WIDTH), jnp.bfloat16),
            pltpu.SemaphoreType.DMA((SLOTS,)),
        ],
        compiler_params=pltpu.CompilerParams(vmem_limit_bytes=8 * 2**20),
        cost_estimate=pl.CostEstimate(
            flops=1_000_000, bytes_accessed=1_000_000, transcendentals=0
        ),
    )(index, source, placed)


def compute(
    tokens, image_keys, image_values, text_len, image_len, counts, old_group, new_group, w_query, w_out
):
    small = (counts, old_group, new_group, text_len, image_len, image_keys, image_values, tokens)
    counts, old_group, new_group, text_len, image_len, image_keys, image_values, tokens = (
        pltpu.with_memory_space_constraint(a, pltpu.HBM) for a in small
    )
    w_far = pltpu.with_memory_space_constraint(w_query, pltpu.HBM)
    *kv, first, came, head0, head1, index = pack(
        counts, old_group, new_group, text_len, image_len, image_keys, image_values
    )

    for k in (1, 3, 2):
        kv[k] = move_group(kv[k], k)
    parts = []
    ready = early(first, tokens, w_far)
    for part in range(2):
        x = list(ready[4 * part : 4 * part + 4])
        for k in (1, 3, 2):
            x[k] = move_group(x[k], k)
        parts.append(x)

    kv_mine, kv_send = choose(came, kv)
    kv_theirs = move_seq(kv_send, "swap")
    block = [jnp.concatenate([kv_mine[j], kv_theirs[j]], axis=2) for j in range(2)]

    pieces = []
    for r in range(2):
        near = [block[r]]
        for k in (1, 2, 3):
            near.append(move_seq(block[r], "near", k))
        own = jnp.stack(near)
        prev = move_seq(own, "far", 1)
        after = move_seq(own, "far", 3)
        opa = move_seq(prev[:2], "far", 1)
        opb = move_seq(after[2:], "far", 3)
        pieces.append((own, prev, after, opa, opb))

    mine, theirs = [], []
    for part in range(2):
        if part:
            q_mine, q_send = late(came, head0, parts[1])
        else:
            q_mine, q_send = project(came, head0, parts[0], w_query)
        mine.append(q_mine)
        theirs.append(move_seq(q_send, "swap"))

    done = []
    for j, head in enumerate((head0, head1)):
        out_mine, out_send = attend(head, (mine[j], theirs[j]), pieces[j], w_out)
        done.append((out_mine, move_seq(out_send, "swap")))
    placed = place_early(index, done[0][0], done[1][0], done[0][1])
    return place_late(index, done[1][1], placed)


def solution(mesh):
    split = P("group", "seq", None)
    return jax.shard_map(
        compute,
        mesh=mesh,
        in_specs=(split,) * 3 + (P(),) * 7,
        out_specs=split,
        check_vma=False,
    )
```

```python
import jax
import jax.numpy as jnp
from jax import lax
from jax.experimental import pallas as pl
from jax.experimental.pallas import tpu as pltpu
from jax.sharding import PartitionSpec as P


HEADS = 16
HEAD_DIM = 128
WIDTH = 2048
GROUPS = 4
SLOTS = 8
TASKS = 6
HALF = 4
RING = 4
CORES = 2
ROWS = 64
KEYS = 8
IMG = 256

masked_score = -1e30
norm_eps = 1e-05


def seq_moves(phase, k):
    pairs = []
    for z in range(RING):
        for y in range(RING):
            for c in range(CORES):
                z2, y2, c2 = z, y, c
                if phase == "swap":
                    c2 = 1 - c
                elif (phase == "near") == (c == 0):
                    z2 = (z + k) % RING
                else:
                    y2 = (y + k) % RING
                pairs.append(((z * RING + y) * CORES + c, (z2 * RING + y2) * CORES + c2))
    return pairs


def move_seq(a, phase, k=1):
    return lax.ppermute(a, "seq", seq_moves(phase, k))


def move_group(a, k):
    return lax.ppermute(a, "group", [(g, (g + k) % GROUPS) for g in range(GROUPS)])


def pack_kernel(
    counts_ref, old_ref, new_ref, text_ref, image_ref, k_ref, v_ref,
    kv0_ref, kv1_ref, kv2_ref, kv3_ref, first_ref, came_ref, head0_ref, head1_ref, index_ref, sem,
):
    group, d = lax.axis_index("group"), lax.axis_index("seq")
    core = d % CORES
    y = (d // CORES) % RING
    z = d // (CORES * RING)
    tasks = range(TASKS)
    count = [counts_ref[t] for t in tasks]
    old = [old_ref[t] for t in tasks]
    new = [new_ref[t] for t in tasks]
    zero = jnp.int32(0)
    start, rank = [], []
    for t in tasks:
        at, before = zero, zero
        for u in range(t):
            at = at + jnp.where(old[u] == old[t], count[u], 0)
            before = before + jnp.where(new[u] == new[t], 1, 0)
        start.append(at)
        rank.append(before)
    copies = []
    for k, out in enumerate((kv0_ref, kv1_ref, kv2_ref, kv3_ref)):
        first = zero
        for t in tasks:
            goes = (old[t] == group) & (new[t] == (group + k) % GROUPS)
            first = jnp.where(goes, start[t], first)
        first_ref[k] = first
        for i, ref in enumerate((k_ref, v_ref)):
            copies.append(
                pltpu.make_async_copy(ref.at[pl.ds(first, HALF)], out.at[i], sem.at[2 * k + i])
            )
            copies[-1].start()
    heads = (head0_ref, head1_ref)
    for head in heads:
        head[0], head[1], head[2] = z, y, core
    amounts = []
    for r in range(2):
        came, amount, base = zero, zero, zero
        for t in tasks:
            mine = (new[t] == group) & (rank[t] == r)
            came = jnp.where(mine, (group - old[t] + GROUPS) % GROUPS, came)
            amount = jnp.where(mine, count[t], amount)
            base = jnp.where(mine, old[t] * SLOTS + start[t], base)
        came_ref[r] = came
        amounts.append(amount)
        for j, head in enumerate(heads):
            sample = 2 * core + j
            there = sample < amount
            slot = jnp.where(there, base + sample, 0)
            head[3 + r] = jnp.where(there, image_ref[slot], IMG)
            text = jnp.where(there, text_ref[slot], 0)
            head[5 + 2 * r] = text - d * ROWS
            head[6 + 2 * r] = text - (d + 1 - 2 * core) * ROWS
    for slot in range(SLOTS):
        second = jnp.where(slot >= amounts[0], 1, 0)
        j = slot - second * amounts[0]
        at = jnp.where(j // 2 == core, 0, 4) + 2 * (j % 2) + second
        index_ref[slot] = jnp.where(slot < amounts[0] + amounts[1], at, -1)
    for copy in copies:
        copy.wait()


def pack(counts, old_group, new_group, text_len, image_len, keys, values):
    smem = pl.BlockSpec(memory_space=pltpu.SMEM)
    vmem = pl.BlockSpec(memory_space=pltpu.VMEM)
    kv = jax.ShapeDtypeStruct((2, HALF, KEYS, WIDTH), jnp.bfloat16)
    ints = [jax.ShapeDtypeStruct((n,), jnp.int32) for n in (4, 2, 9, 9, 8)]
    return pl.pallas_call(
        pack_kernel,
        out_shape=(kv,) * 4 + tuple(ints),
        in_specs=[smem] * 5 + [pl.BlockSpec(memory_space=pltpu.HBM)] * 2,
        out_specs=(vmem,) * 4 + (smem,) * 5,
        scratch_shapes=[pltpu.SemaphoreType.DMA((8,))],
        compiler_params=pltpu.CompilerParams(vmem_limit_bytes=6 * 2**20),
        cost_estimate=pl.CostEstimate(flops=1_000_000, bytes_accessed=2_000_000, transcendentals=0),
    )(counts, old_group, new_group, text_len, image_len, keys, values)


def choose_kernel(came_ref, kv0_ref, kv1_ref, kv2_ref, kv3_ref, mine_ref, send_ref, sem):
    core = lax.axis_index("seq") % CORES
    for r in range(2):
        for k, ref in enumerate((kv0_ref, kv1_ref, kv2_ref, kv3_ref)):

            @pl.when(came_ref[r] == k)
            def _():
                for j in range(2):
                    for side, (at, out) in enumerate(((core, mine_ref), (1 - core, send_ref))):
                        pltpu.make_async_copy(
                            ref.at[:, 2 * at + j], out.at[j, r], sem.at[r, j, side]
                        ).start()

    for r in range(2):
        for j in range(2):
            for side, out in enumerate((mine_ref, send_ref)):
                pltpu.make_async_copy(kv0_ref.at[:, 0], out.at[j, r], sem.at[r, j, side]).wait()


def choose(came, parts):
    out = jax.ShapeDtypeStruct((2, 2, 2, KEYS, WIDTH), jnp.bfloat16)
    return pl.pallas_call(
        choose_kernel,
        out_shape=(out, out),
        in_specs=[pl.BlockSpec(memory_space=pltpu.SMEM)] + [pl.BlockSpec(memory_space=pl.ANY)] * 4,
        out_specs=(pl.BlockSpec(memory_space=pltpu.VMEM),) * 2,
        scratch_shapes=[pltpu.SemaphoreType.DMA((2, 2, 2))],
        compiler_params=pltpu.CompilerParams(vmem_limit_bytes=4 * 2**20),
        cost_estimate=pl.CostEstimate(flops=1_000_000, bytes_accessed=1_000_000, transcendentals=0),
    )(came, *parts)


def scaled_queries(normal, w_ref, n):
    out = jnp.dot(normal, w_ref[:, n * 256 : (n + 1) * 256], preferred_element_type=jnp.float32)
    return (out * HEAD_DIM ** (-0.5)).astype(jnp.bfloat16)


def normalized(x):
    values = x.reshape(-1, WIDTH).astype(jnp.float32)
    centred = values - jnp.mean(values, axis=-1, keepdims=True)
    variance = jnp.mean(centred * centred, axis=-1, keepdims=True)
    return (centred * lax.rsqrt(variance + norm_eps)).astype(jnp.bfloat16)


def start_picks(came_ref, core, parts, mine, send, sem):
    for r in range(2):
        for k, ref in enumerate(parts):

            @pl.when(came_ref[r] == k)
            def _():
                for side, (at, out) in enumerate(((core, mine), (1 - core, send))):
                    pltpu.make_async_copy(ref.at[at], out.at[r], sem.at[r, side]).start()


def wait_picks(parts, side, out, sem):
    for r in range(2):
        pltpu.make_async_copy(parts[0].at[0], out.at[r], sem.at[r, side]).wait()


def project_kernel(
    came_ref, head_ref, x0_ref, x1_ref, x2_ref, x3_ref, w_ref, mine_ref, send_ref, x, normal, sem,
):
    parts = (x0_ref, x1_ref, x2_ref, x3_ref)
    start_picks(came_ref, head_ref[2], parts, x.at[0], x.at[1], sem)
    for side in range(2):
        wait_picks(parts, side, x.at[side], sem)
        normal[side] = normalized(x[side])
    for n in range(8):
        both = normal[...].reshape(4 * ROWS, WIDTH)
        out = scaled_queries(both, w_ref, n).reshape(2, 2, ROWS, 256)
        mine_ref[:, :, n * 256 : (n + 1) * 256] = out[0]
        send_ref[:, :, n * 256 : (n + 1) * 256] = out[1]


def project(came, head, parts, w_query):
    smem = pl.BlockSpec(memory_space=pltpu.SMEM)
    vmem = pl.BlockSpec(memory_space=pltpu.VMEM)
    out = jax.ShapeDtypeStruct((2, ROWS, WIDTH), jnp.bfloat16)
    return pl.pallas_call(
        project_kernel,
        out_shape=(out, out),
        in_specs=[smem, smem] + [pl.BlockSpec(memory_space=pl.ANY)] * 4 + [vmem],
        out_specs=(vmem, vmem),
        scratch_shapes=[
            pltpu.VMEM((2, 2, ROWS, WIDTH), jnp.bfloat16),
            pltpu.VMEM((2, 2 * ROWS, WIDTH), jnp.bfloat16),
            pltpu.SemaphoreType.DMA((2, 2)),
        ],
        compiler_params=pltpu.CompilerParams(vmem_limit_bytes=16 * 2**20),
        cost_estimate=pl.CostEstimate(
            flops=2_150_000_000, bytes_accessed=12_000_000, transcendentals=0
        ),
    )(came, head, *parts, w_query)


def early_kernel(
    first_ref, x_ref, w_hbm, t0_ref, t1_ref, t2_ref, t3_ref, o0_ref, o1_ref, o2_ref, o3_ref,
    x, normal, queries, w_ref, sem, w_sem, t_sem,
):
    second = jnp.int32(0)
    for k in range(GROUPS):
        second = jnp.maximum(second, first_ref[k])
    copies = [
        pltpu.make_async_copy(x_ref.at[at], x.at[i], sem.at[i])
        for i, at in enumerate((1, 3, second + 1, second + 3))
    ]
    blocks = [
        pltpu.make_async_copy(
            w_hbm.at[:, pl.ds(512 * i, 512)], w_ref.at[:, pl.ds(512 * i, 512)], w_sem.at[i]
        )
        for i in range(4)
    ]
    raw = [
        pltpu.make_async_copy(x_ref.at[first_ref[k] + 2 * i], out.at[i], t_sem.at[k, i])
        for k, out in enumerate((t0_ref, t1_ref, t2_ref, t3_ref))
        for i in range(2)
    ]
    for copy in copies + blocks[:2]:
        copy.start()
    for i in range(2):
        copies[2 * i].wait()
        copies[2 * i + 1].wait()
        blocks[2 + i].start()
        normal[2 * ROWS * i : 2 * ROWS * (i + 1)] = normalized(x[2 * i : 2 * i + 2])
    for copy in raw:
        copy.start()
    for n in range(8):
        if n % 2 == 0:
            blocks[n // 2].wait()
        out = scaled_queries(normal[...], w_ref, n)
        queries[:, :, n * 256 : (n + 1) * 256] = out.reshape(4, ROWS, 256)
    for k, out in enumerate((o0_ref, o1_ref, o2_ref, o3_ref)):
        out[...] = queries[pl.ds(jnp.where(first_ref[k] > 0, 2, 0), 2)]
    for copy in raw:
        copy.wait()


def early(first, tokens, w_query):
    vmem = pl.BlockSpec(memory_space=pltpu.VMEM)
    out = jax.ShapeDtypeStruct((2, ROWS, WIDTH), jnp.bfloat16)
    return pl.pallas_call(
        early_kernel,
        out_shape=(out,) * 8,
        in_specs=[
            pl.BlockSpec(memory_space=pltpu.SMEM),
            pl.BlockSpec(memory_space=pltpu.HBM),
            pl.BlockSpec(memory_space=pltpu.HBM),
        ],
        out_specs=(vmem,) * 8,
        scratch_shapes=[
            pltpu.VMEM((4, ROWS, WIDTH), jnp.bfloat16),
            pltpu.VMEM((4 * ROWS, WIDTH), jnp.bfloat16),
            pltpu.VMEM((4, ROWS, WIDTH), jnp.bfloat16),
            pltpu.VMEM((WIDTH, WIDTH), jnp.bfloat16),
            pltpu.SemaphoreType.DMA((4,)),
            pltpu.SemaphoreType.DMA((4,)),
            pltpu.SemaphoreType.DMA((4, 2)),
        ],
        compiler_params=pltpu.CompilerParams(vmem_limit_bytes=20 * 2**20),
        cost_estimate=pl.CostEstimate(
            flops=2_150_000_000, bytes_accessed=12_000_000, transcendentals=0
        ),
    )(first, tokens, w_query)


def late_kernel(came_ref, head_ref, x0_ref, x1_ref, x2_ref, x3_ref, mine_ref, send_ref, sem):
    parts = (x0_ref, x1_ref, x2_ref, x3_ref)
    start_picks(came_ref, head_ref[2], parts, mine_ref, send_ref, sem)
    wait_picks(parts, 0, mine_ref, sem)
    wait_picks(parts, 1, send_ref, sem)


def late(came, head, parts):
    smem = pl.BlockSpec(memory_space=pltpu.SMEM)
    vmem = pl.BlockSpec(memory_space=pltpu.VMEM)
    out = jax.ShapeDtypeStruct((2, ROWS, WIDTH), jnp.bfloat16)
    return pl.pallas_call(
        late_kernel,
        out_shape=(out, out),
        in_specs=[smem, smem] + [pl.BlockSpec(memory_space=pl.ANY)] * 4,
        out_specs=(vmem, vmem),
        scratch_shapes=[pltpu.SemaphoreType.DMA((2, 2))],
        compiler_params=pltpu.CompilerParams(vmem_limit_bytes=4 * 2**20),
        cost_estimate=pl.CostEstimate(flops=1_000_000, bytes_accessed=2_000_000, transcendentals=0),
    )(came, head, *parts)


def attend_kernel(
    head_ref, qm_ref, qt_ref, own_ref, prev_ref, next_ref, opa_ref, opb_ref, w_ref,
    om_ref, ot_ref, ctx,
):
    z, y, core = head_ref[0], head_ref[1], head_ref[2]
    i = lax.broadcasted_iota(jnp.int32, (1, IMG), 1)
    run, which, within = i // 64, (i // 16) & 3, i & 15
    hop = jnp.where(run == 1, 3, jnp.where(run == 2, 1, jnp.where(run == 3, 2, 0)))
    back = 4 - which
    at_z = (z + jnp.where(core == 0, back, hop)) & 3
    at_y = (y + jnp.where(core == 0, hop, back)) & 3
    within = (within & 7) + 8 * jnp.where(within < 8, core, 1 - core)
    key_at = 64 * at_z + 16 * at_y + within
    for r in range(2):
        bias = jnp.where(key_at < head_ref[3 + r], 0.0, masked_score)
        for h in range(HEADS):
            cols = slice(h * HEAD_DIM, (h + 1) * HEAD_DIM)

            def side(kv):
                return jnp.concatenate(
                    [
                        ref[:, r, kv, :, cols].reshape(-1, HEAD_DIM)
                        for ref in (own_ref, prev_ref, next_ref, opa_ref, opb_ref)
                    ],
                    axis=0,
                )

            q = jnp.concatenate([qm_ref[r, :, cols], qt_ref[r, :, cols]], axis=0)
            scores = lax.dot_general(
                q, side(0), (((1,), (1,)), ((), ())), preferred_element_type=jnp.float32
            )
            scores = scores + bias
            top = jnp.max(scores, axis=-1, keepdims=True)
            probs = jnp.exp(scores - top)
            total = jnp.sum(probs, axis=-1, keepdims=True)
            mixed = jnp.dot(
                probs.astype(jnp.bfloat16), side(1), preferred_element_type=jnp.float32
            )
            ctx[2 * ROWS * r : 2 * ROWS * (r + 1), cols] = (mixed * (1.0 / total)).astype(jnp.bfloat16)

    row = lax.broadcasted_iota(jnp.int32, (ROWS, 1), 0)
    for n in range(8):
        cols = slice(n * 256, (n + 1) * 256)
        out = jnp.dot(ctx[...], w_ref[:, cols], preferred_element_type=jnp.float32)
        for r in range(2):
            for side, ref in ((0, om_ref), (1, ot_ref)):
                at = (2 * r + side) * ROWS
                kept = row < head_ref[5 + 2 * r + side]
                ref[r, :, cols] = jnp.where(kept, out[at : at + ROWS], 0.0).astype(jnp.bfloat16)


def attend(head, queries, pieces, w_out):
    vmem = pl.BlockSpec(memory_space=pltpu.VMEM)
    out = jax.ShapeDtypeStruct((2, ROWS, WIDTH), jnp.bfloat16)
    return pl.pallas_call(
        attend_kernel,
        out_shape=(out, out),
        in_specs=[pl.BlockSpec(memory_space=pltpu.SMEM)] + [vmem] * 8,
        out_specs=(vmem, vmem),
        scratch_shapes=[pltpu.VMEM((4 * ROWS, WIDTH), jnp.bfloat16)],
        compiler_params=pltpu.CompilerParams(vmem_limit_bytes=20 * 2**20),
        cost_estimate=pl.CostEstimate(
            flops=3_500_000_000, bytes_accessed=14_000_000, transcendentals=1_000_000
        ),
    )(head, *queries, *pieces, w_out)


def place_kernel(index_ref, m0_ref, m1_ref, t0_ref, t1_ref, out_ref, zeros, sem):
    zeros[...] = jnp.zeros_like(zeros)
    for slot in range(SLOTS):
        source = index_ref[slot]
        for n, ref in enumerate((m0_ref, m1_ref, t0_ref, t1_ref)):
            for j in range(2):

                @pl.when(source == 2 * n + j)
                def _():
                    pltpu.make_async_copy(ref.at[j], out_ref.at[slot], sem.at[slot]).start()

        @pl.when(source < 0)
        def _():
            pltpu.make_async_copy(zeros, out_ref.at[slot], sem.at[slot]).start()

    for slot in range(SLOTS):
        pltpu.make_async_copy(zeros, out_ref.at[slot], sem.at[slot]).wait()


def place(index, m0, m1, t0, t1):
    return pl.pallas_call(
        place_kernel,
        out_shape=jax.ShapeDtypeStruct((SLOTS, ROWS, WIDTH), jnp.bfloat16),
        in_specs=[pl.BlockSpec(memory_space=pltpu.SMEM)]
        + [pl.BlockSpec(memory_space=pltpu.VMEM)] * 4,
        out_specs=pl.BlockSpec(memory_space=pl.ANY),
        scratch_shapes=[
            pltpu.VMEM((ROWS, WIDTH), jnp.bfloat16),
            pltpu.SemaphoreType.DMA((SLOTS,)),
        ],
        compiler_params=pltpu.CompilerParams(vmem_limit_bytes=8 * 2**20),
        cost_estimate=pl.CostEstimate(
            flops=1_000_000, bytes_accessed=4_000_000, transcendentals=0
        ),
    )(index, m0, m1, t0, t1)


def compute(
    tokens, image_keys, image_values, text_len, image_len, counts, old_group, new_group, w_query, w_out
):
    small = (counts, old_group, new_group, text_len, image_len, image_keys, image_values, tokens)
    counts, old_group, new_group, text_len, image_len, image_keys, image_values, tokens = (
        pltpu.with_memory_space_constraint(a, pltpu.HBM) for a in small
    )
    w_far = pltpu.with_memory_space_constraint(w_query, pltpu.HBM)
    *kv, first, came, head0, head1, index = pack(
        counts, old_group, new_group, text_len, image_len, image_keys, image_values
    )

    for k in (1, 3, 2):
        kv[k] = move_group(kv[k], k)
    parts = []
    ready = early(first, tokens, w_far)
    for part in range(2):
        x = list(ready[4 * part : 4 * part + 4])
        for k in (1, 3, 2):
            x[k] = move_group(x[k], k)
        parts.append(x)

    kv_mine, kv_send = choose(came, kv)
    kv_theirs = move_seq(kv_send, "swap")
    block = [jnp.concatenate([kv_mine[j], kv_theirs[j]], axis=2) for j in range(2)]

    pieces = []
    for r in range(2):
        near = [block[r]]
        for k in (1, 2, 3):
            near.append(move_seq(block[r], "near", k))
        own = jnp.stack(near)
        prev = move_seq(own, "far", 1)
        after = move_seq(own, "far", 3)
        opa = move_seq(prev[:2], "far", 1)
        opb = move_seq(after[2:], "far", 3)
        pieces.append((own, prev, after, opa, opb))

    mine, theirs = [], []
    for part in range(2):
        if part:
            q_mine, q_send = late(came, head0, parts[1])
        else:
            q_mine, q_send = project(came, head0, parts[0], w_query)
        mine.append(q_mine)
        theirs.append(move_seq(q_send, "swap"))

    done = []
    for j, head in enumerate((head0, head1)):
        out_mine, out_send = attend(head, (mine[j], theirs[j]), pieces[j], w_out)
        done.append((out_mine, move_seq(out_send, "swap")))
    return place(index, done[0][0], done[1][0], done[0][1], done[1][1])


def solution(mesh):
    split = P("group", "seq", None)
    return jax.shard_map(
        compute,
        mesh=mesh,
        in_specs=(split,) * 3 + (P(),) * 7,
        out_specs=split,
        check_vma=False,
    )
```
